32 devices in a mesh: mem: 4 (over z), lat: 2 (over y), lon: 4 (over x, core).
Axes of the slice: x: 2, y: 2, z: 4, core: 2. Of those that a mesh axis runs over, the one named last changes fastest.
Arguments:
- perturbations: bfloat16 [16, 8, 128, 1024], P('mem', None, 'lat', 'lon'), may hold values from -6 to 6
- increment: float32 [8, 128, 1024], P(None, 'lat', 'lon'), may hold values from -6 to 6
- taper_norm: float32 [8, 128, 1024], P(None, 'lat', 'lon'), may hold values from 1.5 to 6
- kappa: float32 [8], replicated, may hold values from 0.3 to 8
Outputs:
- covariance_product: float32 [8, 128, 1024], P('mem', 'lat', 'lon')
The draws below stay inside these ranges and needn't reach their ends.
All inputs are finite; a program needn't handle non-finite values.
Results may differ from the reference program's by a relative error of at most 0.0003.
Values may be sent and summed in bfloat16 or wider, within the bound.
A program may use at most 64 MiB of HBM per device.

```python
import math
import jax
import jax.numpy as jnp
from jax import lax

LEV = 8
PASSES = 4
SWEEPS = 2
MEMBERS = 16
NLAT = 128
NLON = 1024


def steps_of(rng, extent, split, least, largest):
    def one(dim, blocks):
        draws = jax.random.uniform(jax.random.fold_in(jax.random.fold_in(rng, 6), dim), (blocks,), jnp.float32, least / len(split), largest / len(split))
        return jnp.repeat(jnp.exp(draws), extent[dim] // blocks).reshape((-1,) + (1,) * (len(extent) - dim - 1))

    factor_of = one(*split[0])
    for cut in split[1:]:
        factor_of = factor_of * one(*cut)
    return factor_of


def centred(own_key, dims, deviation, reach, pieces=(), dtype=jnp.bfloat16):
    array = deviation * jax.random.normal(own_key, dims, jnp.float32)
    if pieces:
        array = array * steps_of(own_key, dims, pieces, -0.22, 0.18)
    return jnp.clip(array, -reach, reach).astype(dtype)


def setup_inputs(seed: int = 0) -> dict:
    streams_of = jax.random.split(jax.random.key(seed), 5)
    return {
        "perturbations": centred(streams_of[0], (MEMBERS, LEV, NLAT, NLON), 1.0, 6.0, ((0, 4), (2, 2), (3, 4))),
        "increment": centred(streams_of[1], (LEV, NLAT, NLON), 1.0, 6.0, ((1, 2), (2, 4)), jnp.float32),
        "taper_norm": jnp.clip(jnp.exp(math.log(6.0) - 1.3862944 * jax.random.uniform(streams_of[2], (LEV, NLAT, NLON), jnp.float32) ** steps_of(streams_of[2], (LEV, NLAT, NLON), ((1, 2), (2, 4)), -0.2, 0.2)), 1.5, 6.0),
        "kappa": jnp.clip(jnp.exp(jax.random.uniform(streams_of[3], (LEV,), jnp.float32, math.log(0.3), math.log(8.0))), 0.3, 8.0),
    }


def relax_whole(source, field, weight):
    padded = jnp.pad(field, ((0, 0), (1, 1), (0, 0)))
    padded = jnp.concatenate([padded[:, :, -1:], padded, padded[:, :, :1]], axis=2)
    beside_all = padded[:, 2:, 1:-1] + padded[:, :-2, 1:-1] + padded[:, 1:-1, 2:] + padded[:, 1:-1, :-2]
    return (source + weight * beside_all) / (1.0 + 4.0 * weight)


def diffuse_whole(field, weight):
    for turn in range(2 * PASSES):
        result = field
        for sweep in range(SWEEPS):
            result = relax_whole(field, result, weight)
        field = result
    return field


def reference(perturbations, increment, taper_norm, kappa):
    weight = kappa[:, None, None]

    def add_member(total, member):
        values = member.astype(jnp.float32)
        spread = taper_norm * (values * increment)
        tapered = taper_norm * diffuse_whole(spread, weight)
        return total + values * tapered, None

    total, unused = lax.scan(add_member, jnp.zeros(increment.shape, jnp.float32), perturbations)
    return total / (MEMBERS - 1)
```

```python
import functools

import jax
import jax.numpy as jnp
import numpy as np
from jax import lax
from jax.experimental import pallas as pl
from jax.experimental.pallas import tpu as pltpu
from jax.sharding import PartitionSpec as P

PASSES = 4
SWEEPS = 2
DEPTH = 2 * PASSES * SWEEPS
SUB = 8
LANES = 128
MESH = pl.DeviceIdType.MESH


def roll(value, shift):
    shift = shift % LANES
    return value if shift == 0 else pltpu.roll(value, shift, value.ndim - 1)


def halves(matrix):
    high = np.asarray(matrix, np.float64).astype(jnp.bfloat16)
    return high, (matrix - high.astype(np.float64)).astype(jnp.bfloat16)


def sine(n):
    order = np.arange(1, n + 1)
    basis = np.sqrt(2.0 / (n + 1)) * np.sin(np.pi * np.outer(order, order) / (n + 1))
    return basis, 2.0 * np.cos(np.pi * order / (n + 1))


def column_tables():
    basis, own = sine(LANES)
    lanes = np.arange(LANES)
    into, back = [], []
    for shift in (DEPTH, LANES // 2, -DEPTH):
        high, low = halves(basis[(lanes + shift) % LANES])
        into.append(np.block([[high, low], [high, low]]))
        back.append(np.block([[high.T, low.T], [high.T, low.T]]))
    return np.stack(into), np.stack(back), own


def row_tables(rows, sides, columns):
    full = rows + sides * DEPTH
    kinds = [[], [0, 1], [0, 1, 2]][sides] or [None]
    into, back, own = [], [], []
    for kind in kinds:
        above = sides == 2 and kind > 0 or sides == 1 and kind == 1
        below = sides == 2 and kind < 2 or sides == 1 and kind == 0
        start = DEPTH if above else 0
        size = rows + start + (DEPTH if below else 0)
        basis, eig = sine(size)
        spots = [np.arange(start, start + rows)]
        for side, there in enumerate((above, below)):
            first = 0 if side == 0 else start + rows
            if there:
                spots.append(np.arange(first, first + DEPTH))
            elif sides == 2:
                spots.append(np.full(DEPTH, -1))
        spots = np.concatenate(spots)
        table = np.zeros((full, full))
        table[:size] = np.where(spots < 0, 0.0, basis[:, spots])
        high, low = halves(table)
        into.append(np.concatenate([high, low, high], 1))
        high, low = halves(table.T[:rows])
        back.append(np.concatenate([high, low, high], 1))
        sums = np.zeros((full, LANES))
        sums[:size] = eig[:, None] + columns
        own.append(sums.astype(np.float32))
    return np.stack(into), np.stack(back), np.stack(own)


def split(value):
    high = value.astype(jnp.bfloat16)
    return high, (value - high.astype(jnp.float32)).astype(jnp.bfloat16)


def kernel(
    sizes, kappa, pert, inc, taper, into_c, back_c, into_r, back_r, eigen, out,
    g, pack, rlon, cpack, rcor, rlat_p, rlat_g, lhs, mid, rhs, part, rpart,
    lon_send, lon_recv, latp_send, latp_recv, latg_send, latg_recv,
    cor_send, cor_recv, part_send, part_recv,
):
    n_mem, n_lat, n_lon = sizes
    mem, lat, lon = lax.axis_index("mem"), lax.axis_index("lat"), lax.axis_index("lon")
    members, levels, rows, cols = pert.shape
    per = levels // n_mem
    sides = min(n_lat - 1, 2)
    full = rows + sides * DEPTH
    kind = jnp.where(lat == 0, 0, jnp.where(lat == n_lat - 1, sides, 1)) if sides else 0
    lane = lax.broadcasted_iota(jnp.int32, (SUB, LANES), 1)
    lon_to = [lax.rem(lon + 1, n_lon), lax.rem(lon + n_lon - 1, n_lon)]
    lat_to = [lat + 1, lat - 1]
    sends = [lat < n_lat - 1, lat > 0]
    gets = [lat > 0, lat < n_lat - 1]
    edge = [rows - DEPTH, 0]
    slot = [0, 1 if sides == 2 else 0]

    def group(t):
        return lax.rem(mem + 1 + t, n_mem)

    def remote(src, dst, send, recv, **where):
        return pltpu.make_async_remote_copy(
            src_ref=src, dst_ref=dst, send_sem=send, recv_sem=recv,
            device_id=where, device_id_type=MESH,
        )

    def lon_copy(t, b):
        return remote(pack.at[b, t], rlon.at[b, t], lon_send.at[b, t], lon_recv.at[b, t],
                      mem=mem, lat=lat, lon=lon_to[b])

    def cor_copy(t, a, b):
        return remote(cpack.at[a, b, t], rcor.at[slot[a], b, t], cor_send.at[a, b, t],
                      cor_recv.at[slot[a], b, t], mem=mem, lat=lat_to[a], lon=lon_to[b])

    def latp_copy(t, a):
        return remote(pert.at[:, pl.ds(group(t) * per, per), pl.ds(edge[a], DEPTH), :],
                      rlat_p.at[slot[a], t], latp_send.at[a, t], latp_recv.at[slot[a], t],
                      mem=mem, lat=lat_to[a], lon=lon)

    def latg_copy(t, a):
        return remote(g.at[pl.ds(group(t) * per, per), pl.ds(edge[a], DEPTH), :],
                      rlat_g.at[slot[a], t], latg_send.at[a, t], latg_recv.at[slot[a], t],
                      mem=mem, lat=lat_to[a], lon=lon)

    def part_copy(t):
        return remote(part.at[t], rpart.at[t], part_send.at[t], part_recv.at[t],
                      mem=group(t), lat=lat, lon=lon)

    barrier = pltpu.get_barrier_semaphore()

    def greet(**where):
        pl.semaphore_signal(barrier, inc=1, device_id=where, device_id_type=MESH)

    for b in range(2):
        greet(mem=mem, lat=lat, lon=lon_to[b])
    for t in range(n_mem - 1):
        greet(mem=group(t), lat=lat, lon=lon)
    for a in range(2):
        @pl.when(sends[a])
        def _():
            greet(mem=mem, lat=lat_to[a], lon=lon)
            for b in range(2):
                greet(mem=mem, lat=lat_to[a], lon=lon_to[b])

    g[...] = taper[...] * inc[...]

    beside = sum(jnp.where(s, 1, 0) for s in sends)
    pl.semaphore_wait(barrier, 2 + (n_mem - 1) + 3 * beside)

    def send_group(t, carry):
        e = group(t)
        for a in range(2):
            @pl.when(sends[a])
            def _():
                latg_copy(t, a).start()
                latp_copy(t, a).start()
        for b, column in enumerate((cols - LANES, 0)):
            source = LANES - DEPTH if b == 0 else 0
            corners = [[None] * (SUB * 2 * DEPTH // LANES) for _ in range(2)]
            for s in range(SUB):
                m, l = s // per, s % per
                w = pert[m, e * per + l, :, pl.ds(column, LANES)].astype(jnp.float32)
                w = w * g[e * per + l, :, pl.ds(column, LANES)]
                acc = None
                for q in range(rows // SUB):
                    v = roll(w[q * SUB : (q + 1) * SUB], q * DEPTH - source)
                    acc = v if acc is None else jnp.where(lane >= q * DEPTH, v, acc)
                pack[b, t, s] = acc
                each = LANES // (2 * DEPTH)
                j, i = s // each, s % each
                for a in range(2):
                    start = (edge[a] // SUB) * DEPTH
                    v = roll(acc, i * 2 * DEPTH - start)
                    old = corners[a][j]
                    corners[a][j] = v if old is None else jnp.where(lane >= i * 2 * DEPTH, v, old)
            for a in range(2):
                for j, v in enumerate(corners[a]):
                    cpack[a, b, t, j] = v
            lon_copy(t, b).start()
            for a in range(2):
                @pl.when(sends[a])
                def _():
                    cor_copy(t, a, b).start()
        return carry

    lax.fori_loop(0, n_mem, send_group, 0)

    lane1 = lax.broadcasted_iota(jnp.int32, (2 * SUB, LANES), 1)

    def place(at, x, low, high):
        x0, x1 = x[:, :LANES], x[:, LANES:]
        views = (
            jnp.where(lane1 < LANES - DEPTH, x0, low),
            jnp.where(lane1 < LANES // 2, x1, x0),
            jnp.where(lane1 < DEPTH, high, x1),
        )
        for k, view in enumerate(views):
            first, second = split(view)
            lhs[k, at : at + 2 * SUB, :LANES] = first
            lhs[k, at : at + 2 * SUB, LANES:] = second

    def pair(left, right, at):
        low = [roll(left, LANES - DEPTH - at - h * DEPTH) for h in range(2)]
        high = [roll(right, -at - h * DEPTH) for h in range(2)]
        return jnp.concatenate(low, 0), jnp.concatenate(high, 0)

    def windows(t):
        e = group(t)
        for s in range(SUB):
            m, l = s // per, s % per
            left, right = rlon[0, t, s], rlon[1, t, s]
            for q in range(0, rows // SUB, 2):
                r = slice(q * SUB, (q + 2) * SUB)
                w = pert[m, e * per + l, r].astype(jnp.float32) * g[e * per + l, r]
                place(s * full + q * SUB, w, *pair(left, right, q * DEPTH))
        each = LANES // (2 * DEPTH)
        for a in range(sides):
            def fill():
                for s in range(SUB):
                    m, l = s // per, s % per
                    j, i = s // each, s % each
                    w = rlat_p[a, t, m, l].astype(jnp.float32) * rlat_g[a, t, l]
                    left, right = rcor[a, 0, t, j], rcor[a, 1, t, j]
                    place(s * full + rows + a * DEPTH, w, *pair(left, right, i * 2 * DEPTH))

            if sides == 1:
                fill()
            else:
                pl.when(gets[a])(fill)

                @pl.when(jnp.logical_not(gets[a]))
                def _():
                    zero = jnp.zeros((DEPTH, 2 * LANES), jnp.bfloat16)
                    for s in range(SUB):
                        for k in range(3):
                            at = s * full + rows + a * DEPTH
                            lhs[k, at : at + DEPTH] = zero

    def damping(l):
        k1 = jnp.full((SUB, LANES), kappa[l], jnp.float32)
        scale = 1.0 / (1.0 + 4.0 * k1)
        tiles = []
        for i in range(0, full, SUB):
            n = k1 * eigen[kind, i : i + SUB]
            p = jnp.ones_like(n)
            for _ in range(SWEEPS):
                p = scale * (1.0 + n * p)
            for _ in range((2 * PASSES).bit_length() - 1):
                p = p * p
            tiles.append(p)
        return jnp.concatenate(tiles, 0)

    def dot(x, y):
        return jnp.dot(x, y, preferred_element_type=jnp.float32)

    def transform(t):
        e = group(t)
        for k in range(3):
            c = dot(lhs[k], into_c[k])
            for s in range(SUB):
                z = c[s * full : (s + 1) * full]
                first, second = split(z[:, :LANES] + z[:, LANES:])
                lanes = slice(k * LANES, (k + 1) * LANES)
                mid[s, :full, lanes] = first
                mid[s, full:, lanes] = second
        for l in range(per):
            p = damping(e * per + l)
            p = jnp.concatenate([p, p, p], 1)
            for m in range(members):
                s = m * per + l
                first, second = mid[s, :full], mid[s, full:]
                c = dot(into_r[kind], jnp.concatenate([first, first, second], 0))
                first, second = split(c * p)
                c = dot(back_r[kind], jnp.concatenate([first, first, second], 0))
                first, second = split(c)
                for k in range(3):
                    lanes = slice(k * LANES, (k + 1) * LANES)
                    rhs[k, s * rows : (s + 1) * rows, :LANES] = first[:, lanes]
                    rhs[k, s * rows : (s + 1) * rows, LANES:] = second[:, lanes]

    def work(t, carry):
        e = group(t)
        for b in range(2):
            lon_copy(t, b).wait_recv()
        for a in range(2):
            @pl.when(gets[a])
            def _():
                latg_copy(t, a).wait_recv()
                latp_copy(t, a).wait_recv()
                for b in range(2):
                    cor_copy(t, a, b).wait_recv()
        windows(t)
        transform(t)
        lane2 = lax.broadcasted_iota(jnp.int32, (rows, LANES), 1)
        sums = [[0.0, 0.0] for _ in range(per)]
        y = [dot(rhs[k], back_c[k]) for k in range(3)]
        y = [v[:, :LANES] + v[:, LANES:] for v in y]
        for l in range(per):
            for m in range(members):
                s = m * per + l
                r = slice(s * rows, (s + 1) * rows)
                v = pert[m, e * per + l].astype(jnp.float32)
                low = jnp.where(lane2 < LANES - 2 * DEPTH, y[0][r], y[1][r])
                high = jnp.where(lane2 < 2 * DEPTH, y[1][r], y[2][r])
                sums[l][0] = sums[l][0] + v[:, :LANES] * low
                sums[l][1] = sums[l][1] + v[:, LANES:] * high
            tap = taper[e * per + l] * (1.0 / (members * n_mem - 1))
            part[t, l, :, :LANES] = sums[l][0] * tap[:, :LANES]
            part[t, l, :, LANES:] = sums[l][1] * tap[:, LANES:]

        @pl.when(t < n_mem - 1)
        def _():
            part_copy(t).start()

        return carry

    lax.fori_loop(0, n_mem, work, 0)
    total = part[n_mem - 1]
    for t in range(n_mem - 1):
        part_copy(t).wait_recv()
        total = total + rpart[t]
    out[...] = total

    def drain(t, carry):
        for b in range(2):
            lon_copy(t, b).wait_send()
        for a in range(2):
            @pl.when(sends[a])
            def _():
                latg_copy(t, a).wait_send()
                latp_copy(t, a).wait_send()
                for b in range(2):
                    cor_copy(t, a, b).wait_send()
        return carry

    lax.fori_loop(0, n_mem, drain, 0)
    for t in range(n_mem - 1):
        part_copy(t).wait_send()


def local(sizes, perturbations, increment, taper_norm, kappa):
    n_mem, n_lat, n_lon = sizes
    members, levels, rows, cols = perturbations.shape
    per = levels // n_mem
    assert members * per == SUB and cols == 2 * LANES and rows * DEPTH == SUB * LANES
    f32 = jnp.float32
    sides = min(n_lat - 1, 2)
    full = rows + sides * DEPTH
    tiles = SUB * 2 * DEPTH // LANES
    into_c, back_c, own = column_tables()
    tables = (into_c, back_c) + row_tables(rows, sides, own)
    dma = pltpu.SemaphoreType.DMA
    vmem = pl.BlockSpec(memory_space=pltpu.VMEM)
    return pl.pallas_call(
        functools.partial(kernel, sizes),
        out_shape=jax.ShapeDtypeStruct((per, rows, cols), f32),
        in_specs=[pl.BlockSpec(memory_space=pltpu.SMEM)] + [vmem] * 8,
        out_specs=vmem,
        scratch_shapes=[
            pltpu.VMEM((levels, rows, cols), f32),
            pltpu.VMEM((2, n_mem, SUB, SUB, LANES), f32),
            pltpu.VMEM((2, n_mem, SUB, SUB, LANES), f32),
            pltpu.VMEM((2, 2, n_mem, tiles, SUB, LANES), f32),
            pltpu.VMEM((2, 2, n_mem, tiles, SUB, LANES), f32),
            pltpu.VMEM((2, n_mem, members, per, DEPTH, cols), jnp.bfloat16),
            pltpu.VMEM((2, n_mem, per, DEPTH, cols), f32),
            pltpu.VMEM((3, SUB * full, 2 * LANES), jnp.bfloat16),
            pltpu.VMEM((SUB, 2 * full, 3 * LANES), jnp.bfloat16),
            pltpu.VMEM((3, SUB * rows, 2 * LANES), jnp.bfloat16),
            pltpu.VMEM((n_mem, per, rows, cols), f32),
            pltpu.VMEM((n_mem - 1, per, rows, cols), f32),
            dma((2, n_mem)), dma((2, n_mem)),
            dma((2, n_mem)), dma((2, n_mem)),
            dma((2, n_mem)), dma((2, n_mem)),
            dma((2, 2, n_mem)), dma((2, 2, n_mem)),
            dma((n_mem - 1,)), dma((n_mem - 1,)),
        ],
        compiler_params=pltpu.CompilerParams(collective_id=0, has_side_effects=True),
    )(kappa, perturbations, increment, taper_norm, *map(jnp.asarray, tables))


def solution(mesh):
    sizes = tuple(mesh.shape[name] for name in ("mem", "lat", "lon"))
    return jax.shard_map(
        functools.partial(local, sizes),
        mesh=mesh,
        in_specs=(P("mem", None, "lat", "lon"), P(None, "lat", "lon"), P(None, "lat", "lon"), P()),
        out_specs=P("mem", "lat", "lon"),
        check_vma=False,
    )
```

```python
import functools

import jax
import jax.numpy as jnp
import numpy as np
from jax import lax
from jax.experimental import pallas as pl
from jax.experimental.pallas import tpu as pltpu
from jax.sharding import PartitionSpec as P

PASSES = 4
SWEEPS = 2
DEPTH = 2 * PASSES * SWEEPS
SUB = 8
LANES = 128
MESH = pl.DeviceIdType.MESH
ROOT = 4
PEAK = 2.0 ** (126 / 2**ROOT)


def roll(value, shift):
    shift = shift % LANES
    return value if shift == 0 else pltpu.roll(value, shift, value.ndim - 1)


def halves(matrix):
    high = np.asarray(matrix, np.float64).astype(jnp.bfloat16)
    return high, (matrix - high.astype(np.float64)).astype(jnp.bfloat16)


def sine(n):
    order = np.arange(1, n + 1)
    basis = np.sqrt(2.0 / (n + 1)) * np.sin(np.pi * np.outer(order, order) / (n + 1))
    return basis, 2.0 * np.cos(np.pi * order / (n + 1))


def column_tables():
    basis, own = sine(LANES)
    lanes = np.arange(LANES)
    into, back = [], []
    for shift in (DEPTH, LANES // 2, -DEPTH):
        high, low = halves(basis[(lanes + shift) % LANES])
        into.append(np.block([[high, low], [high, low]]))
        back.append(np.block([[high.T, low.T], [high.T, low.T]]))
    return np.stack(into), np.stack(back), own


def row_tables(rows, sides, columns):
    full = rows + sides * DEPTH
    kinds = [[], [0, 1], [0, 1, 2]][sides] or [None]
    into, back, own = [], [], []
    for kind in kinds:
        above = sides == 2 and kind > 0 or sides == 1 and kind == 1
        below = sides == 2 and kind < 2 or sides == 1 and kind == 0
        start = DEPTH if above else 0
        size = rows + start + (DEPTH if below else 0)
        basis, eig = sine(size)
        spots = [np.arange(start, start + rows)]
        for side, there in enumerate((above, below)):
            first = 0 if side == 0 else start + rows
            if there:
                spots.append(np.arange(first, first + DEPTH))
            elif sides == 2:
                spots.append(np.full(DEPTH, -1))
        spots = np.concatenate(spots)
        table = np.zeros((full, full))
        table[:size] = np.where(spots < 0, 0.0, basis[:, spots])
        high, low = halves(table)
        into.append(np.concatenate([high, low, high], 1))
        high, low = halves(table.T[:rows])
        back.append(np.concatenate([high, low, high], 1))
        sums = np.zeros((full, LANES))
        sums[:size] = eig[:, None] + columns
        own.append(sums.astype(np.float32))
    return np.stack(into), np.stack(back), np.stack(own)


def split(value):
    high = value.astype(jnp.bfloat16)
    return high, (value - high.astype(jnp.float32)).astype(jnp.bfloat16)


def top(value):
    tiles = [
        jnp.abs(value[i : i + SUB, j : j + LANES])
        for i in range(0, value.shape[0], SUB)
        for j in range(0, value.shape[1], LANES)
    ]
    while len(tiles) > 1:
        tiles = [jnp.maximum(*tiles[i : i + 2]) if tiles[i + 1 :] else tiles[i] for i in range(0, len(tiles), 2)]
    return tiles[0]


def spread(tile, like):
    tile = jnp.concatenate([tile] * (like.shape[1] // LANES), 1)
    return jnp.concatenate([tile] * (like.shape[0] // SUB), 0)


def encode(value, scale):
    power = value * spread(PEAK / scale, value)
    negative = power < 0.0
    for _ in range(ROOT):
        power = power * power
    return jnp.where(negative, -power, power).astype(jnp.bfloat16)


def decode(coded, scale):
    coded = coded.astype(jnp.float32)
    value = jnp.exp2(jnp.log2(jnp.abs(coded)) * (0.5**ROOT)) * spread(scale * (1.0 / PEAK), coded)
    return jnp.where(coded < 0.0, -value, value)


def kernel(
    sizes, kappa, pert_h, inc_h, taper_h, into_c_h, back_c_h, into_r_h, back_r_h, eigen_h, out,
    pert, inc, taper, into_c, back_c, into_r, back_r, eigen, load, g, pack, rlon, cpack, rcor, rlat_p, rlat_g, lhs, mid, rhs, own, part, rpart,
    lon_send, lon_recv, latp_send, latp_recv, latg_send, latg_recv,
    cor_send, cor_recv, part_send, part_recv,
):
    n_mem, n_lat, n_lon = sizes
    mem, lat, lon = lax.axis_index("mem"), lax.axis_index("lat"), lax.axis_index("lon")
    members, levels, rows, cols = pert.shape
    per = levels // n_mem
    sides = min(n_lat - 1, 2)
    full = rows + sides * DEPTH
    kind = jnp.where(lat == 0, 0, jnp.where(lat == n_lat - 1, sides, 1)) if sides else 0
    lane = lax.broadcasted_iota(jnp.int32, (SUB, LANES), 1)
    lon_to = [lax.rem(lon + 1, n_lon), lax.rem(lon + n_lon - 1, n_lon)]
    lat_to = [lat + 1, lat - 1]
    sends = [lat < n_lat - 1, lat > 0]
    gets = [lat > 0, lat < n_lat - 1]
    edge = [rows - DEPTH, 0]
    slot = [0, 1 if sides == 2 else 0]

    def group(t):
        return lax.rem(mem + 1 + t, n_mem)

    def remote(src, dst, send, recv, **where):
        return pltpu.make_async_remote_copy(
            src_ref=src, dst_ref=dst, send_sem=send, recv_sem=recv,
            device_id=where, device_id_type=MESH,
        )

    def lon_copy(t, b):
        return remote(pack.at[b, t], rlon.at[b, t], lon_send.at[b, t], lon_recv.at[b, t],
                      mem=mem, lat=lat, lon=lon_to[b])

    def cor_copy(t, a, b):
        return remote(cpack.at[a, b, t], rcor.at[slot[a], b, t], cor_send.at[a, b, t],
                      cor_recv.at[slot[a], b, t], mem=mem, lat=lat_to[a], lon=lon_to[b])

    def latp_copy(t, a):
        return remote(pert.at[:, pl.ds(group(t) * per, per), pl.ds(edge[a], DEPTH), :],
                      rlat_p.at[slot[a], t], latp_send.at[a, t], latp_recv.at[slot[a], t],
                      mem=mem, lat=lat_to[a], lon=lon)

    def latg_copy(t, a):
        return remote(g.at[pl.ds(group(t) * per, per), pl.ds(edge[a], DEPTH), :],
                      rlat_g.at[slot[a], t], latg_send.at[a, t], latg_recv.at[slot[a], t],
                      mem=mem, lat=lat_to[a], lon=lon)

    def part_copy(t):
        return remote(part.at[t], rpart.at[t], part_send.at[t], part_recv.at[t],
                      mem=group(t), lat=lat, lon=lon)

    loads = [
        pltpu.make_async_copy(source, target, load.at[i])
        for i, (source, target) in enumerate((
            (inc_h, inc), (taper_h, taper), (pert_h, pert), (into_c_h, into_c), (into_r_h, into_r),
            (eigen_h, eigen), (back_r_h, back_r), (back_c_h, back_c),
        ))
    ]
    barrier = pltpu.get_barrier_semaphore()

    def greet(**where):
        pl.semaphore_signal(barrier, inc=1, device_id=where, device_id_type=MESH)

    for b in range(2):
        greet(mem=mem, lat=lat, lon=lon_to[b])
    for t in range(n_mem - 1):
        greet(mem=group(t), lat=lat, lon=lon)
    for a in range(2):
        @pl.when(sends[a])
        def _():
            greet(mem=mem, lat=lat_to[a], lon=lon)
            for b in range(2):
                greet(mem=mem, lat=lat_to[a], lon=lon_to[b])

    for copy in loads:
        copy.start()
    for copy in loads[:2]:
        copy.wait()
    g[...] = taper[...] * inc[...]
    loads[2].wait()

    beside = sum(jnp.where(s, 1, 0) for s in sends)
    pl.semaphore_wait(barrier, 2 + (n_mem - 1) + 3 * beside)

    def send_group(t, carry):
        e = group(t)
        for a in range(2):
            @pl.when(sends[a])
            def _():
                latg_copy(t, a).start()
                latp_copy(t, a).start()
        for b, column in enumerate((cols - LANES, 0)):
            source = LANES - DEPTH if b == 0 else 0
            corners = [[None] * (SUB * 2 * DEPTH // LANES) for _ in range(2)]
            for s in range(SUB):
                m, l = s // per, s % per
                w = pert[m, e * per + l, :, pl.ds(column, LANES)].astype(jnp.float32)
                w = w * g[e * per + l, :, pl.ds(column, LANES)]
                acc = None
                for q in range(rows // SUB):
                    v = roll(w[q * SUB : (q + 1) * SUB], q * DEPTH - source)
                    acc = v if acc is None else jnp.where(lane >= q * DEPTH, v, acc)
                pack[b, t, s] = acc
                each = LANES // (2 * DEPTH)
                j, i = s // each, s % each
                for a in range(2):
                    start = (edge[a] // SUB) * DEPTH
                    v = roll(acc, i * 2 * DEPTH - start)
                    old = corners[a][j]
                    corners[a][j] = v if old is None else jnp.where(lane >= i * 2 * DEPTH, v, old)
            for a in range(2):
                for j, v in enumerate(corners[a]):
                    cpack[a, b, t, j] = v
            lon_copy(t, b).start()
            for a in range(2):
                @pl.when(sends[a])
                def _():
                    cor_copy(t, a, b).start()
        return carry

    lax.fori_loop(0, n_mem, send_group, 0)
    for copy in loads[3:]:
        copy.wait()

    lane1 = lax.broadcasted_iota(jnp.int32, (2 * SUB, LANES), 1)

    def place(at, x, low, high):
        x0, x1 = x[:, :LANES], x[:, LANES:]
        views = (
            jnp.where(lane1 < LANES - DEPTH, x0, low),
            jnp.where(lane1 < LANES // 2, x1, x0),
            jnp.where(lane1 < DEPTH, high, x1),
        )
        for k, view in enumerate(views):
            first, second = split(view)
            lhs[k, at : at + 2 * SUB, :LANES] = first
            lhs[k, at : at + 2 * SUB, LANES:] = second

    def pair(left, right, at):
        low = [roll(left, LANES - DEPTH - at - h * DEPTH) for h in range(2)]
        high = [roll(right, -at - h * DEPTH) for h in range(2)]
        return jnp.concatenate(low, 0), jnp.concatenate(high, 0)

    def windows(t):
        e = group(t)
        for s in range(SUB):
            m, l = s // per, s % per
            left, right = rlon[0, t, s], rlon[1, t, s]
            for q in range(0, rows // SUB, 2):
                r = slice(q * SUB, (q + 2) * SUB)
                w = pert[m, e * per + l, r].astype(jnp.float32) * g[e * per + l, r]
                place(s * full + q * SUB, w, *pair(left, right, q * DEPTH))
        each = LANES // (2 * DEPTH)
        for a in range(sides):
            def fill():
                for s in range(SUB):
                    m, l = s // per, s % per
                    j, i = s // each, s % each
                    w = rlat_p[a, t, m, l].astype(jnp.float32) * rlat_g[a, t, l]
                    left, right = rcor[a, 0, t, j], rcor[a, 1, t, j]
                    place(s * full + rows + a * DEPTH, w, *pair(left, right, i * 2 * DEPTH))

            if sides == 1:
                fill()
            else:
                pl.when(gets[a])(fill)

                @pl.when(jnp.logical_not(gets[a]))
                def _():
                    zero = jnp.zeros((DEPTH, 2 * LANES), jnp.bfloat16)
                    for s in range(SUB):
                        for k in range(3):
                            at = s * full + rows + a * DEPTH
                            lhs[k, at : at + DEPTH] = zero

    def damping(l):
        k1 = jnp.full((SUB, LANES), kappa[l], jnp.float32)
        scale = 1.0 / (1.0 + 4.0 * k1)
        tiles = []
        for i in range(0, full, SUB):
            n = k1 * eigen[kind, i : i + SUB]
            p = jnp.ones_like(n)
            for _ in range(SWEEPS):
                p = scale * (1.0 + n * p)
            for _ in range((2 * PASSES).bit_length() - 1):
                p = p * p
            tiles.append(p)
        return jnp.concatenate(tiles, 0)

    def dot(x, y):
        return jnp.dot(x, y, preferred_element_type=jnp.float32)

    def transform(t):
        e = group(t)
        for k in range(3):
            c = dot(lhs[k], into_c[k])
            for s in range(SUB):
                z = c[s * full : (s + 1) * full]
                first, second = split(z[:, :LANES] + z[:, LANES:])
                lanes = slice(k * LANES, (k + 1) * LANES)
                mid[s, :full, lanes] = first
                mid[s, full:, lanes] = second
        for l in range(per):
            p = damping(e * per + l)
            p = jnp.concatenate([p, p, p], 1)
            for m in range(members):
                s = m * per + l
                first, second = mid[s, :full], mid[s, full:]
                c = dot(into_r[kind], jnp.concatenate([first, first, second], 0))
                first, second = split(c * p)
                c = dot(back_r[kind], jnp.concatenate([first, first, second], 0))
                first, second = split(c)
                for k in range(3):
                    lanes = slice(k * LANES, (k + 1) * LANES)
                    rhs[k, s * rows : (s + 1) * rows, :LANES] = first[:, lanes]
                    rhs[k, s * rows : (s + 1) * rows, LANES:] = second[:, lanes]

    def work(t, carry):
        e = group(t)
        for b in range(2):
            lon_copy(t, b).wait_recv()
        for a in range(2):
            @pl.when(gets[a])
            def _():
                latg_copy(t, a).wait_recv()
                latp_copy(t, a).wait_recv()
                for b in range(2):
                    cor_copy(t, a, b).wait_recv()
        windows(t)
        transform(t)
        lane2 = lax.broadcasted_iota(jnp.int32, (rows, LANES), 1)
        sums = [[0.0, 0.0] for _ in range(per)]
        y = [dot(rhs[k], back_c[k]) for k in range(3)]
        y = [v[:, :LANES] + v[:, LANES:] for v in y]
        for l in range(per):
            for m in range(members):
                s = m * per + l
                r = slice(s * rows, (s + 1) * rows)
                v = pert[m, e * per + l].astype(jnp.float32)
                low = jnp.where(lane2 < LANES - 2 * DEPTH, y[0][r], y[1][r])
                high = jnp.where(lane2 < 2 * DEPTH, y[1][r], y[2][r])
                sums[l][0] = sums[l][0] + v[:, :LANES] * low
                sums[l][1] = sums[l][1] + v[:, LANES:] * high
            tap = taper[e * per + l] * (1.0 / (members * n_mem - 1))
            total = jnp.concatenate(sums[l], 1) * tap
            own[l] = total

        @pl.when(t < n_mem - 1)
        def _():
            value = own[...].reshape(per * rows, cols)
            scale = jnp.maximum(top(value), 1e-30).astype(jnp.bfloat16)
            tile = jnp.concatenate([scale, scale], 0)
            part[t, per * rows :] = jnp.concatenate([tile] * (cols // LANES), 1)
            part[t, : per * rows] = encode(value, scale.astype(jnp.float32))
            part_copy(t).start()

        return carry

    lax.fori_loop(0, n_mem, work, 0)
    total = own[...].reshape(per * rows, cols)
    for t in range(n_mem - 1):
        part_copy(t).wait_recv()
        scale = rpart[t, per * rows :, :LANES].astype(jnp.float32)[:SUB]
        total = total + decode(rpart[t, : per * rows], scale)
    out[...] = total.reshape(per, rows, cols)

    def drain(t, carry):
        for b in range(2):
            lon_copy(t, b).wait_send()
        for a in range(2):
            @pl.when(sends[a])
            def _():
                latg_copy(t, a).wait_send()
                latp_copy(t, a).wait_send()
                for b in range(2):
                    cor_copy(t, a, b).wait_send()
        return carry

    lax.fori_loop(0, n_mem, drain, 0)
    for t in range(n_mem - 1):
        part_copy(t).wait_send()


def local(sizes, perturbations, increment, taper_norm, kappa):
    n_mem, n_lat, n_lon = sizes
    members, levels, rows, cols = perturbations.shape
    per = levels // n_mem
    assert members * per == SUB and cols == 2 * LANES and rows * DEPTH == SUB * LANES
    f32 = jnp.float32
    sides = min(n_lat - 1, 2)
    full = rows + sides * DEPTH
    tiles = SUB * 2 * DEPTH // LANES
    into_c, back_c, eig = column_tables()
    tables = (into_c, back_c) + row_tables(rows, sides, eig)
    arrays = (perturbations, increment, taper_norm, *map(jnp.asarray, tables))
    dma = pltpu.SemaphoreType.DMA
    vmem = pl.BlockSpec(memory_space=pltpu.VMEM)
    return pl.pallas_call(
        functools.partial(kernel, sizes),
        out_shape=pltpu.VMEM((per, rows, cols), f32),
        in_specs=[pl.BlockSpec(memory_space=pltpu.SMEM)] + [pl.BlockSpec(memory_space=pl.ANY)] * len(arrays),
        out_specs=vmem,
        scratch_shapes=[pltpu.VMEM(array.shape, array.dtype) for array in arrays] + [
            dma((len(arrays),)),
            pltpu.VMEM((levels, rows, cols), f32),
            pltpu.VMEM((2, n_mem, SUB, SUB, LANES), f32),
            pltpu.VMEM((2, n_mem, SUB, SUB, LANES), f32),
            pltpu.VMEM((2, 2, n_mem, tiles, SUB, LANES), f32),
            pltpu.VMEM((2, 2, n_mem, tiles, SUB, LANES), f32),
            pltpu.VMEM((2, n_mem, members, per, DEPTH, cols), jnp.bfloat16),
            pltpu.VMEM((2, n_mem, per, DEPTH, cols), f32),
            pltpu.VMEM((3, SUB * full, 2 * LANES), jnp.bfloat16),
            pltpu.VMEM((SUB, 2 * full, 3 * LANES), jnp.bfloat16),
            pltpu.VMEM((3, SUB * rows, 2 * LANES), jnp.bfloat16),
            pltpu.VMEM((per, rows, cols), f32),
            pltpu.VMEM((n_mem - 1, per * rows + 2 * SUB, cols), jnp.bfloat16),
            pltpu.VMEM((n_mem - 1, per * rows + 2 * SUB, cols), jnp.bfloat16),
            dma((2, n_mem)), dma((2, n_mem)),
            dma((2, n_mem)), dma((2, n_mem)),
            dma((2, n_mem)), dma((2, n_mem)),
            dma((2, 2, n_mem)), dma((2, 2, n_mem)),
            dma((n_mem - 1,)), dma((n_mem - 1,)),
        ],
        compiler_params=pltpu.CompilerParams(collective_id=0, has_side_effects=True),
    )(kappa, *arrays)


def solution(mesh):
    sizes = tuple(mesh.shape[name] for name in ("mem", "lat", "lon"))
    return jax.shard_map(
        functools.partial(local, sizes),
        mesh=mesh,
        in_specs=(P("mem", None, "lat", "lon"), P(None, "lat", "lon"), P(None, "lat", "lon"), P()),
        out_specs=P("mem", "lat", "lon"),
        check_vma=False,
    )
```

```python
import functools

import jax
import jax.numpy as jnp
import numpy as np
from jax import lax
from jax.experimental import pallas as pl
from jax.experimental.pallas import tpu as pltpu
from jax.sharding import PartitionSpec as P

PASSES = 4
SWEEPS = 2
DEPTH = 2 * PASSES * SWEEPS
SUB = 8
LANES = 128
MESH = pl.DeviceIdType.MESH
ROOT = 4
PEAK = 2.0 ** (126 / 2**ROOT)
CORNER = 2.0 ** (126 / 4) / 6.0**3


def roll(value, shift):
    shift = shift % LANES
    return value if shift == 0 else pltpu.roll(value, shift, value.ndim - 1)


def halves(matrix):
    high = np.asarray(matrix, np.float64).astype(jnp.bfloat16)
    return high, (matrix - high.astype(np.float64)).astype(jnp.bfloat16)


def sine(n):
    order = np.arange(1, n + 1)
    basis = np.sqrt(2.0 / (n + 1)) * np.sin(np.pi * np.outer(order, order) / (n + 1))
    return basis, 2.0 * np.cos(np.pi * order / (n + 1))


def column_tables():
    basis, own = sine(LANES)
    lanes = np.arange(LANES)
    into, back = [], []
    for shift in (DEPTH, LANES // 2, -DEPTH):
        high, low = halves(basis[(lanes + shift) % LANES])
        into.append(np.block([[high, low], [high, low]]))
        back.append(np.block([[high.T, low.T], [high.T, low.T]]))
    return np.stack(into), np.stack(back), own


def row_tables(rows, sides, columns):
    full = rows + sides * DEPTH
    kinds = [[], [0, 1], [0, 1, 2]][sides] or [None]
    into, back, own = [], [], []
    for kind in kinds:
        above = sides == 2 and kind > 0 or sides == 1 and kind == 1
        below = sides == 2 and kind < 2 or sides == 1 and kind == 0
        start = DEPTH if above else 0
        size = rows + start + (DEPTH if below else 0)
        basis, eig = sine(size)
        spots = [np.arange(start, start + rows)]
        for side, there in enumerate((above, below)):
            first = 0 if side == 0 else start + rows
            if there:
                spots.append(np.arange(first, first + DEPTH))
            elif sides == 2:
                spots.append(np.full(DEPTH, -1))
        spots = np.concatenate(spots)
        table = np.zeros((full, full))
        table[:size] = np.where(spots < 0, 0.0, basis[:, spots])
        high, low = halves(table)
        into.append(np.concatenate([high, low, high], 1))
        high, low = halves(table.T[:rows])
        back.append(np.concatenate([high, low, high], 1))
        sums = np.zeros((full, LANES))
        sums[:size] = eig[:, None] + columns
        own.append(sums.astype(np.float32))
    return np.stack(into), np.stack(back), np.stack(own)


def split(value):
    high = value.astype(jnp.bfloat16)
    return high, (value - high.astype(jnp.float32)).astype(jnp.bfloat16)


def top(value):
    tiles = [
        jnp.abs(value[i : i + SUB, j : j + LANES])
        for i in range(0, value.shape[0], SUB)
        for j in range(0, value.shape[1], LANES)
    ]
    while len(tiles) > 1:
        tiles = [jnp.maximum(*tiles[i : i + 2]) if tiles[i + 1 :] else tiles[i] for i in range(0, len(tiles), 2)]
    return tiles[0]


def spread(tile, like):
    tile = jnp.concatenate([tile] * (like.shape[1] // LANES), 1)
    return jnp.concatenate([tile] * (like.shape[0] // SUB), 0)


def power(value, squares):
    negative = value < 0.0
    for _ in range(squares):
        value = value * value
    return jnp.where(negative, -value, value).astype(jnp.bfloat16)


def root(coded, order):
    coded = coded.astype(jnp.float32)
    value = jnp.exp2(jnp.log2(jnp.abs(coded)) * (1.0 / order))
    return jnp.where(coded < 0.0, -value, value)


def encode(message, value):
    scale = jnp.maximum(top(value), 1e-30).astype(jnp.bfloat16)
    message[: 2 * SUB] = jnp.concatenate([scale, scale], 0)
    coded = power(value * spread(PEAK / scale.astype(jnp.float32), value), ROOT)
    for i in range(value.shape[1] // LANES):
        message[pl.ds(2 * SUB + i * value.shape[0], value.shape[0])] = coded[:, i * LANES : (i + 1) * LANES]


def decode(message, start, count):
    scale = message[: 2 * SUB].astype(jnp.float32)[:SUB] * (1.0 / PEAK)
    value = root(message[pl.ds(2 * SUB + start, count)], 2**ROOT)
    return value * spread(scale, value)


def kernel(
    sizes, kappa, pert_h, inc_h, taper_h, into_c_h, back_c_h, into_r_h, back_r_h, eigen_h, out,
    pert, inc, taper, into_c, back_c, into_r, back_r, eigen, load, g, pack, rlon, cpack, rcor, epack, rlat, lhs, mid, rhs, own, part, rpart,
    lon_send, lon_recv, lat_send, lat_recv, cor_send, cor_recv, part_send, part_recv,
):
    n_mem, n_lat, n_lon = sizes
    mem, lat, lon = lax.axis_index("mem"), lax.axis_index("lat"), lax.axis_index("lon")
    members, levels, rows, cols = pert.shape
    per = levels // n_mem
    sides = min(n_lat - 1, 2)
    full = rows + sides * DEPTH
    kind = jnp.where(lat == 0, 0, jnp.where(lat == n_lat - 1, sides, 1)) if sides else 0
    lane = lax.broadcasted_iota(jnp.int32, (SUB, LANES), 1)
    lon_to = [lax.rem(lon + 1, n_lon), lax.rem(lon + n_lon - 1, n_lon)]
    lat_to = [lat + 1, lat - 1]
    sends = [lat < n_lat - 1, lat > 0]
    gets = [lat > 0, lat < n_lat - 1]
    edge = [rows - DEPTH, 0]
    slot = [0, 1 if sides == 2 else 0]

    def group(t):
        near = jnp.minimum(mem, n_mem - 1 - mem)
        far = n_mem - 1 - 2 * near
        step = jnp.maximum(t - far, 0)
        away = near - lax.div(step, 2)
        paired = jnp.where(lax.rem(step, 2) == 0, mem - away, mem + away)
        return jnp.where(t < far, jnp.where(2 * mem < n_mem, n_mem - 1 - t, t), paired)

    def spot(here, there):
        return lax.rem(here - there + n_mem - 1, n_mem)

    def remote(src, dst, send, recv, **where):
        return pltpu.make_async_remote_copy(
            src_ref=src, dst_ref=dst, send_sem=send, recv_sem=recv,
            device_id=where, device_id_type=MESH,
        )

    def lon_copy(t, b):
        return remote(pack.at[b, t], rlon.at[b, t], lon_send.at[b, t], lon_recv.at[b, t],
                      mem=mem, lat=lat, lon=lon_to[b])

    def cor_copy(t, a, b):
        return remote(cpack.at[a, b, t], rcor.at[slot[a], b, t], cor_send.at[a, b, t],
                      cor_recv.at[slot[a], b, t], mem=mem, lat=lat_to[a], lon=lon_to[b])

    def lat_copy(t, a):
        return remote(epack.at[slot[a], t], rlat.at[slot[a], t], lat_send.at[a, t], lat_recv.at[slot[a], t],
                      mem=mem, lat=lat_to[a], lon=lon)

    def part_copy(t):
        e = group(t)
        i = spot(mem, e)
        return remote(part.at[t], rpart.at[i], part_send.at[t], part_recv.at[i],
                      mem=e, lat=lat, lon=lon)

    def part_come(i):
        return remote(part.at[i], rpart.at[i], part_send.at[i], part_recv.at[i],
                      mem=lax.rem(mem + 1, n_mem), lat=lat, lon=lon)

    loads = [
        pltpu.make_async_copy(source, target, load.at[i])
        for i, (source, target) in enumerate((
            (inc_h, inc), (taper_h, taper), (pert_h, pert), (into_c_h, into_c), (into_r_h, into_r),
            (eigen_h, eigen), (back_r_h, back_r), (back_c_h, back_c),
        ))
    ]
    barrier = pltpu.get_barrier_semaphore()

    def greet(**where):
        pl.semaphore_signal(barrier, inc=1, device_id=where, device_id_type=MESH)

    for b in range(2):
        greet(mem=mem, lat=lat, lon=lon_to[b])
    for t in range(n_mem - 1):
        greet(mem=group(t), lat=lat, lon=lon)
    for a in range(2):
        @pl.when(sends[a])
        def _():
            greet(mem=mem, lat=lat_to[a], lon=lon)
            for b in range(2):
                greet(mem=mem, lat=lat_to[a], lon=lon_to[b])

    for copy in loads:
        copy.start()
    for copy in loads[:2]:
        copy.wait()
    g[...] = taper[...] * inc[...]
    loads[2].wait()

    beside = sum(jnp.where(s, 1, 0) for s in sends)
    pl.semaphore_wait(barrier, 2 + (n_mem - 1) + 3 * beside)

    def send_group(t, carry):
        e = group(t)
        for a in range(2):
            @pl.when(sends[a])
            def _():
                r = pl.ds(edge[a], DEPTH)
                w = [
                    pert[s // per, e * per + s % per, r, :].astype(jnp.float32) * g[e * per + s % per, r, :]
                    for s in range(SUB)
                ]
                encode(epack.at[slot[a], t], jnp.concatenate(w, 0))
                lat_copy(t, a).start()
        for b, column in enumerate((cols - LANES, 0)):
            source = LANES - DEPTH if b == 0 else 0
            corners = [[None] * (SUB * 2 * DEPTH // LANES) for _ in range(2)]
            edges = []
            for s in range(SUB):
                m, l = s // per, s % per
                w = pert[m, e * per + l, :, pl.ds(column, LANES)].astype(jnp.float32)
                w = w * g[e * per + l, :, pl.ds(column, LANES)]
                acc = None
                for q in range(rows // SUB):
                    v = roll(w[q * SUB : (q + 1) * SUB], q * DEPTH - source)
                    acc = v if acc is None else jnp.where(lane >= q * DEPTH, v, acc)
                edges.append(acc)
                each = LANES // (2 * DEPTH)
                j, i = s // each, s % each
                for a in range(2):
                    start = (edge[a] // SUB) * DEPTH
                    v = roll(acc, i * 2 * DEPTH - start)
                    old = corners[a][j]
                    corners[a][j] = v if old is None else jnp.where(lane >= i * 2 * DEPTH, v, old)
            encode(pack.at[b, t], jnp.concatenate(edges, 0))
            lon_copy(t, b).start()
            for a in range(2):
                @pl.when(sends[a])
                def _():
                    cpack[a, b, t] = power(jnp.concatenate(corners[a], 0) * CORNER, 2)
                    cor_copy(t, a, b).start()
        return carry

    lax.fori_loop(0, n_mem, send_group, 0)
    for copy in loads[3:]:
        copy.wait()

    lane1 = lax.broadcasted_iota(jnp.int32, (2 * SUB, LANES), 1)

    def place(at, x, low, high):
        x0, x1 = x[:, :LANES], x[:, LANES:]
        views = (
            jnp.where(lane1 < LANES - DEPTH, x0, low),
            jnp.where(lane1 < LANES // 2, x1, x0),
            jnp.where(lane1 < DEPTH, high, x1),
        )
        for k, view in enumerate(views):
            first, second = split(view)
            lhs[k, at : at + 2 * SUB, :LANES] = first
            lhs[k, at : at + 2 * SUB, LANES:] = second

    def pair(left, right, at):
        low = [roll(left, LANES - DEPTH - at - h * DEPTH) for h in range(2)]
        high = [roll(right, -at - h * DEPTH) for h in range(2)]
        return jnp.concatenate(low, 0), jnp.concatenate(high, 0)

    def windows(t):
        e = group(t)
        left, right = (decode(rlon.at[b, t], 0, SUB * SUB) for b in range(2))
        for s in range(SUB):
            m, l = s // per, s % per
            mine = slice(s * SUB, (s + 1) * SUB)
            for q in range(0, rows // SUB, 2):
                r = slice(q * SUB, (q + 2) * SUB)
                w = pert[m, e * per + l, r].astype(jnp.float32) * g[e * per + l, r]
                place(s * full + q * SUB, w, *pair(left[mine], right[mine], q * DEPTH))

    def margins(t):
        each = LANES // (2 * DEPTH)
        for a in range(sides):
            def fill():
                left, right = (root(rcor[a, b, t], 4) * (1.0 / CORNER) for b in range(2))
                for s in range(SUB):
                    j, i = s // each, s % each
                    mine = slice(j * SUB, (j + 1) * SUB)
                    w = [decode(rlat.at[a, t], (k * SUB + s) * DEPTH, DEPTH) for k in range(cols // LANES)]
                    place(s * full + rows + a * DEPTH, jnp.concatenate(w, 1),
                          *pair(left[mine], right[mine], i * 2 * DEPTH))

            if sides == 1:
                fill()
            else:
                pl.when(gets[a])(fill)

                @pl.when(jnp.logical_not(gets[a]))
                def _():
                    zero = jnp.zeros((DEPTH, 2 * LANES), jnp.bfloat16)
                    for s in range(SUB):
                        for k in range(3):
                            at = s * full + rows + a * DEPTH
                            lhs[k, at : at + DEPTH] = zero

    def damping(l):
        k1 = jnp.full((SUB, LANES), kappa[l], jnp.float32)
        scale = 1.0 / (1.0 + 4.0 * k1)
        tiles = []
        for i in range(0, full, SUB):
            n = k1 * eigen[kind, i : i + SUB]
            p = jnp.ones_like(n)
            for _ in range(SWEEPS):
                p = scale * (1.0 + n * p)
            for _ in range((2 * PASSES).bit_length() - 1):
                p = p * p
            tiles.append(p)
        return jnp.concatenate(tiles, 0)

    def dot(x, y):
        return jnp.dot(x, y, preferred_element_type=jnp.float32)

    def transform(t):
        e = group(t)
        for k in range(3):
            c = dot(lhs[k], into_c[k])
            for s in range(SUB):
                z = c[s * full : (s + 1) * full]
                first, second = split(z[:, :LANES] + z[:, LANES:])
                lanes = slice(k * LANES, (k + 1) * LANES)
                mid[s, :full, lanes] = first
                mid[s, full:, lanes] = second
        for l in range(per):
            p = damping(e * per + l)
            p = jnp.concatenate([p, p, p], 1)
            batch = [m * per + l for m in range(members)]
            first = jnp.concatenate([mid[s, :full] for s in batch], 1)
            second = jnp.concatenate([mid[s, full:] for s in batch], 1)
            c = dot(into_r[kind], jnp.concatenate([first, first, second], 0))
            first, second = split(c * jnp.concatenate([p] * members, 1))
            c = dot(back_r[kind], jnp.concatenate([first, first, second], 0))
            first, second = split(c)
            for i, s in enumerate(batch):
                for k in range(3):
                    lanes = slice((3 * i + k) * LANES, (3 * i + k + 1) * LANES)
                    rhs[k, s * rows : (s + 1) * rows, :LANES] = first[:, lanes]
                    rhs[k, s * rows : (s + 1) * rows, LANES:] = second[:, lanes]

    def work(t, carry):
        e = group(t)
        for b in range(2):
            lon_copy(t, b).wait_recv()
        windows(t)
        for a in range(2):
            @pl.when(gets[a])
            def _():
                lat_copy(t, a).wait_recv()
                for b in range(2):
                    cor_copy(t, a, b).wait_recv()
        margins(t)
        transform(t)
        lane2 = lax.broadcasted_iota(jnp.int32, (rows, LANES), 1)
        sums = [[0.0, 0.0] for _ in range(per)]
        y = [dot(rhs[k], back_c[k]) for k in range(3)]
        y = [v[:, :LANES] + v[:, LANES:] for v in y]
        for l in range(per):
            for m in range(members):
                s = m * per + l
                r = slice(s * rows, (s + 1) * rows)
                v = pert[m, e * per + l].astype(jnp.float32)
                low = jnp.where(lane2 < LANES - 2 * DEPTH, y[0][r], y[1][r])
                high = jnp.where(lane2 < 2 * DEPTH, y[1][r], y[2][r])
                sums[l][0] = sums[l][0] + v[:, :LANES] * low
                sums[l][1] = sums[l][1] + v[:, LANES:] * high
            tap = taper[e * per + l] * (1.0 / (members * n_mem - 1))
            total = jnp.concatenate(sums[l], 1) * tap
            own[l] = total

        @pl.when(t < n_mem - 1)
        def _():
            encode(part.at[t], own[...].reshape(per * rows, cols))
            part_copy(t).start()

        return carry

    lax.fori_loop(0, n_mem, work, 0)
    for i in range(n_mem - 1):
        part_come(i).wait_recv()
    for k in range(cols // LANES):
        lanes = slice(k * LANES, (k + 1) * LANES)
        total = own[:, :, lanes].reshape(per * rows, LANES)
        for i in range(n_mem - 1):
            total = total + decode(rpart.at[i], k * per * rows, per * rows)
        out[:, :, lanes] = total.reshape(per, rows, LANES)

    def drain(t, carry):
        for b in range(2):
            lon_copy(t, b).wait_send()
        for a in range(2):
            @pl.when(sends[a])
            def _():
                lat_copy(t, a).wait_send()
                for b in range(2):
                    cor_copy(t, a, b).wait_send()
        return carry

    lax.fori_loop(0, n_mem, drain, 0)
    for t in range(n_mem - 1):
        part_copy(t).wait_send()


def local(sizes, perturbations, increment, taper_norm, kappa):
    n_mem, n_lat, n_lon = sizes
    members, levels, rows, cols = perturbations.shape
    per = levels // n_mem
    assert members * per == SUB and cols == 2 * LANES and rows * DEPTH == SUB * LANES
    f32, bf16 = jnp.float32, jnp.bfloat16
    sides = min(n_lat - 1, 2)
    full = rows + sides * DEPTH
    tiles = SUB * 2 * DEPTH // LANES
    into_c, back_c, eig = column_tables()
    tables = (into_c, back_c) + row_tables(rows, sides, eig)
    arrays = (perturbations, increment, taper_norm, *map(jnp.asarray, tables))
    dma = pltpu.SemaphoreType.DMA
    vmem = pl.BlockSpec(memory_space=pltpu.VMEM)
    return pl.pallas_call(
        functools.partial(kernel, sizes),
        out_shape=pltpu.VMEM((per, rows, cols), f32),
        in_specs=[pl.BlockSpec(memory_space=pltpu.SMEM)] + [pl.BlockSpec(memory_space=pl.ANY)] * len(arrays),
        out_specs=vmem,
        scratch_shapes=[pltpu.VMEM(array.shape, array.dtype) for array in arrays] + [
            dma((len(arrays),)),
            pltpu.VMEM((levels, rows, cols), f32),
            pltpu.VMEM((2, n_mem, 2 * SUB + SUB * SUB, LANES), bf16),
            pltpu.VMEM((2, n_mem, 2 * SUB + SUB * SUB, LANES), bf16),
            pltpu.VMEM((2, 2, n_mem, tiles * SUB, LANES), bf16),
            pltpu.VMEM((2, 2, n_mem, tiles * SUB, LANES), bf16),
            pltpu.VMEM((2, n_mem, 2 * SUB + SUB * DEPTH * cols // LANES, LANES), bf16),
            pltpu.VMEM((2, n_mem, 2 * SUB + SUB * DEPTH * cols // LANES, LANES), bf16),
            pltpu.VMEM((3, SUB * full, 2 * LANES), jnp.bfloat16),
            pltpu.VMEM((SUB, 2 * full, 3 * LANES), jnp.bfloat16),
            pltpu.VMEM((3, SUB * rows, 2 * LANES), jnp.bfloat16),
            pltpu.VMEM((per, rows, cols), f32),
            pltpu.VMEM((n_mem - 1, 2 * SUB + per * rows * cols // LANES, LANES), bf16),
            pltpu.VMEM((n_mem - 1, 2 * SUB + per * rows * cols // LANES, LANES), bf16),
            dma((2, n_mem)), dma((2, n_mem)),
            dma((2, n_mem)), dma((2, n_mem)),
            dma((2, 2, n_mem)), dma((2, 2, n_mem)),
            dma((n_mem - 1,)), dma((n_mem - 1,)),
        ],
        compiler_params=pltpu.CompilerParams(collective_id=0, has_side_effects=True),
    )(kappa, *arrays)


def solution(mesh):
    sizes = tuple(mesh.shape[name] for name in ("mem", "lat", "lon"))
    return jax.shard_map(
        functools.partial(local, sizes),
        mesh=mesh,
        in_specs=(P("mem", None, "lat", "lon"), P(None, "lat", "lon"), P(None, "lat", "lon"), P()),
        out_specs=P("mem", "lat", "lon"),
        check_vma=False,
    )
```

```python
import functools

import jax
import jax.numpy as jnp
import numpy as np
from jax import lax
from jax.experimental import pallas as pl
from jax.experimental.pallas import tpu as pltpu
from jax.sharding import PartitionSpec as P

PASSES = 4
SWEEPS = 2
DEPTH = 2 * PASSES * SWEEPS
SUB = 8
LANES = 128
MESH = pl.DeviceIdType.MESH
ROOT = 4
PEAK = 2.0 ** (126 / 2**ROOT)
CORNER = 2.0 ** (126 / 4) / 6.0**3


def roll(value, shift):
    shift = shift % LANES
    return value if shift == 0 else pltpu.roll(value, shift, value.ndim - 1)


def halves(matrix):
    high = np.asarray(matrix, np.float64).astype(jnp.bfloat16)
    return high, (matrix - high.astype(np.float64)).astype(jnp.bfloat16)


def sine(n):
    order = np.arange(1, n + 1)
    basis = np.sqrt(2.0 / (n + 1)) * np.sin(np.pi * np.outer(order, order) / (n + 1))
    return basis, 2.0 * np.cos(np.pi * order / (n + 1))


def column_tables():
    basis, own = sine(LANES)
    lanes = np.arange(LANES)
    into, back = [], []
    for shift in (DEPTH, LANES // 2, -DEPTH):
        high, low = halves(basis[(lanes + shift) % LANES])
        into.append(np.block([[high, low], [high, low]]))
        back.append(np.block([[high.T, low.T], [high.T, low.T]]))
    return np.stack(into), np.stack(back), own


def row_tables(rows, sides, columns):
    full = rows + sides * DEPTH
    kinds = [[], [0, 1], [0, 1, 2]][sides] or [None]
    into, back, own = [], [], []
    for kind in kinds:
        above = sides == 2 and kind > 0 or sides == 1 and kind == 1
        below = sides == 2 and kind < 2 or sides == 1 and kind == 0
        start = DEPTH if above else 0
        size = rows + start + (DEPTH if below else 0)
        basis, eig = sine(size)
        spots = [np.arange(start, start + rows)]
        for side, there in enumerate((above, below)):
            first = 0 if side == 0 else start + rows
            if there:
                spots.append(np.arange(first, first + DEPTH))
            elif sides == 2:
                spots.append(np.full(DEPTH, -1))
        spots = np.concatenate(spots)
        table = np.zeros((full, full))
        table[:size] = np.where(spots < 0, 0.0, basis[:, spots])
        high, low = halves(table)
        into.append(np.concatenate([high, low, high], 1))
        high, low = halves(table.T[:rows])
        back.append(np.concatenate([high, low, high], 1))
        sums = np.zeros((full, LANES))
        sums[:size] = eig[:, None] + columns
        own.append(sums.astype(np.float32))
    return np.stack(into), np.stack(back), np.stack(own)


def split(value):
    high = value.astype(jnp.bfloat16)
    return high, (value - high.astype(jnp.float32)).astype(jnp.bfloat16)


def top(value):
    tiles = [
        jnp.abs(value[i : i + SUB, j : j + LANES])
        for i in range(0, value.shape[0], SUB)
        for j in range(0, value.shape[1], LANES)
    ]
    while len(tiles) > 1:
        tiles = [jnp.maximum(*tiles[i : i + 2]) if tiles[i + 1 :] else tiles[i] for i in range(0, len(tiles), 2)]
    return tiles[0]


def spread(tile, like):
    tile = jnp.concatenate([tile] * (like.shape[1] // LANES), 1)
    return jnp.concatenate([tile] * (like.shape[0] // SUB), 0)


def power(value, squares):
    negative = value < 0.0
    for _ in range(squares):
        value = value * value
    return jnp.where(negative, -value, value).astype(jnp.bfloat16)


def root(coded, order):
    coded = coded.astype(jnp.float32)
    value = jnp.exp2(jnp.log2(jnp.abs(coded)) * (1.0 / order))
    return jnp.where(coded < 0.0, -value, value)


def encode(message, value):
    scale = jnp.maximum(top(value), 1e-30).astype(jnp.bfloat16)
    message[: 2 * SUB] = jnp.concatenate([scale, scale], 0)
    coded = power(value * spread(PEAK / scale.astype(jnp.float32), value), ROOT)
    for i in range(value.shape[1] // LANES):
        message[pl.ds(2 * SUB + i * value.shape[0], value.shape[0])] = coded[:, i * LANES : (i + 1) * LANES]


def decode(message, start, count):
    scale = message[: 2 * SUB].astype(jnp.float32)[:SUB] * (1.0 / PEAK)
    value = root(message[pl.ds(2 * SUB + start, count)], 2**ROOT)
    return value * spread(scale, value)


def kernel(
    sizes, kappa, pert_h, inc_h, taper_h, into_c_h, back_c_h, into_r_h, back_r_h, eigen_h, out,
    pert, inc, taper, into_c, back_c, into_r, back_r, eigen, load, load_c, ready, g, pack, rlon, cpack, rcor, epack, rlat, lhs, lhm, mid, rhs, own, part, rpart,
    lon_send, lon_recv, lat_send, lat_recv, cor_send, cor_recv, part_send, part_recv,
):
    n_mem, n_lat, n_lon = sizes
    mem, lat, lon = lax.axis_index("mem"), lax.axis_index("lat"), lax.axis_index("lon")
    members, levels, rows, cols = pert.shape
    per = levels // n_mem
    sides = min(n_lat - 1, 2)
    full = rows + sides * DEPTH
    kind = jnp.where(lat == 0, 0, jnp.where(lat == n_lat - 1, sides, 1)) if sides else 0
    lane = lax.broadcasted_iota(jnp.int32, (SUB, LANES), 1)
    lon_to = [lax.rem(lon + 1, n_lon), lax.rem(lon + n_lon - 1, n_lon)]
    lat_to = [lat + 1, lat - 1]
    sends = [lat < n_lat - 1, lat > 0]
    gets = [lat > 0, lat < n_lat - 1]
    edge = [rows - DEPTH, 0]
    slot = [0, 1 if sides == 2 else 0]

    def group(t):
        near = jnp.minimum(mem, n_mem - 1 - mem)
        ends = jnp.where(lax.rem(t, 2) == 0, lax.div(t, 2), n_mem - 1 - lax.div(t, 2))
        rest = jnp.where(2 * mem >= n_mem, t - near, n_mem - 1 - t + near)
        return jnp.where(t < 2 * near, ends, rest)

    def spot(here, there):
        return lax.rem(here - there + n_mem - 1, n_mem)

    def remote(src, dst, send, recv, **where):
        return pltpu.make_async_remote_copy(
            src_ref=src, dst_ref=dst, send_sem=send, recv_sem=recv,
            device_id=where, device_id_type=MESH,
        )

    def lon_copy(t, b):
        return remote(pack.at[b, t], rlon.at[b, t], lon_send.at[b, t], lon_recv.at[b, t],
                      mem=mem, lat=lat, lon=lon_to[b])

    def cor_copy(t, a, b):
        return remote(cpack.at[a, b, t], rcor.at[slot[a], b, t], cor_send.at[a, b, t],
                      cor_recv.at[slot[a], b, t], mem=mem, lat=lat_to[a], lon=lon_to[b])

    def lat_copy(t, a):
        return remote(epack.at[slot[a], t], rlat.at[slot[a], t], lat_send.at[a, t], lat_recv.at[slot[a], t],
                      mem=mem, lat=lat_to[a], lon=lon)

    def part_copy(t):
        e = group(t)
        i = spot(mem, e)
        return remote(part.at[t], rpart.at[i], part_send.at[t], part_recv.at[i],
                      mem=e, lat=lat, lon=lon)

    def part_come(i):
        return remote(part.at[i], rpart.at[i], part_send.at[i], part_recv.at[i],
                      mem=lax.rem(mem + 1, n_mem), lat=lat, lon=lon)

    def pieces(t):
        mine = pl.ds(group(t) * per, per)
        return [
            pltpu.make_async_copy(source, target, load.at[i, t])
            for i, (source, target) in enumerate((
                (inc_h.at[mine], inc.at[mine]), (taper_h.at[mine], taper.at[mine]),
                (pert_h.at[:, mine], pert.at[:, mine]),
            ))
        ]

    tables = [
        pltpu.make_async_copy(source, target, load_c.at[i])
        for i, (source, target) in enumerate((
            (into_c_h, into_c), (into_r_h, into_r), (eigen_h, eigen), (back_r_h, back_r), (back_c_h, back_c),
        ))
    ]
    for copy in pieces(0) + tables[:1] + pieces(1) + tables[1:]:
        copy.start()
    for t in range(2, n_mem):
        for copy in pieces(t):
            copy.start()

    barrier = pltpu.get_barrier_semaphore()

    def greet(**where):
        pl.semaphore_signal(barrier, inc=1, device_id=where, device_id_type=MESH)

    for b in range(2):
        greet(mem=mem, lat=lat, lon=lon_to[b])
    for d in range(1, n_mem):
        @pl.when(mem + d < n_mem)
        def _():
            greet(mem=mem + d, lat=lat, lon=lon)
    for a in range(2):
        @pl.when(sends[a])
        def _():
            greet(mem=mem, lat=lat_to[a], lon=lon)
            for b in range(2):
                greet(mem=mem, lat=lat_to[a], lon=lon_to[b])

    beside = sum(jnp.where(s, 1, 0) for s in sends)
    pl.semaphore_wait(barrier, 2 + mem + 3 * beside)
    for d in range(1, n_mem):
        @pl.when(mem >= d)
        def _():
            pl.semaphore_signal(ready, inc=1, device_id=dict(mem=mem - d, lat=lat, lon=lon), device_id_type=MESH)

    def send_group(t, carry):
        e = group(t)
        for copy in pieces(t):
            copy.wait()
        mine = pl.ds(e * per, per)
        g[mine] = taper[mine] * inc[mine]
        for a in range(2):
            @pl.when(sends[a])
            def _():
                r = pl.ds(edge[a], DEPTH)
                w = [
                    pert[s // per, e * per + s % per, r, :].astype(jnp.float32) * g[e * per + s % per, r, :]
                    for s in range(SUB)
                ]
                encode(epack.at[slot[a], t], jnp.concatenate(w, 0))
                lat_copy(t, a).start()
        for b, column in enumerate((cols - LANES, 0)):
            source = LANES - DEPTH if b == 0 else 0
            corners = [[None] * (SUB * 2 * DEPTH // LANES) for _ in range(2)]
            edges = []
            for s in range(SUB):
                m, l = s // per, s % per
                w = pert[m, e * per + l, :, pl.ds(column, LANES)].astype(jnp.float32)
                w = w * g[e * per + l, :, pl.ds(column, LANES)]
                acc = None
                for q in range(rows // SUB):
                    v = roll(w[q * SUB : (q + 1) * SUB], q * DEPTH - source)
                    acc = v if acc is None else jnp.where(lane >= q * DEPTH, v, acc)
                edges.append(acc)
                each = LANES // (2 * DEPTH)
                j, i = s // each, s % each
                for a in range(2):
                    start = (edge[a] // SUB) * DEPTH
                    v = roll(acc, i * 2 * DEPTH - start)
                    old = corners[a][j]
                    corners[a][j] = v if old is None else jnp.where(lane >= i * 2 * DEPTH, v, old)
            encode(pack.at[b, t], jnp.concatenate(edges, 0))
            lon_copy(t, b).start()
            for a in range(2):
                @pl.when(sends[a])
                def _():
                    cpack[a, b, t] = power(jnp.concatenate(corners[a], 0) * CORNER, 2)
                    cor_copy(t, a, b).start()
        return carry

    lax.fori_loop(0, n_mem, send_group, 0)
    for copy in tables:
        copy.wait()

    lane1 = lax.broadcasted_iota(jnp.int32, (2 * SUB, LANES), 1)

    def place(lhs, at, x, low, high):
        x0, x1 = x[:, :LANES], x[:, LANES:]
        views = (
            jnp.where(lane1 < LANES - DEPTH, x0, low),
            jnp.where(lane1 < LANES // 2, x1, x0),
            jnp.where(lane1 < DEPTH, high, x1),
        )
        for k, view in enumerate(views):
            first, second = split(view)
            lhs[k, at : at + 2 * SUB, :LANES] = first
            lhs[k, at : at + 2 * SUB, LANES:] = second

    def pair(left, right, at):
        low = [roll(left, LANES - DEPTH - at - h * DEPTH) for h in range(2)]
        high = [roll(right, -at - h * DEPTH) for h in range(2)]
        return jnp.concatenate(low, 0), jnp.concatenate(high, 0)

    def windows(t):
        e = group(t)
        left, right = (decode(rlon.at[b, t], 0, SUB * SUB) for b in range(2))
        for s in range(SUB):
            m, l = s // per, s % per
            mine = slice(s * SUB, (s + 1) * SUB)
            for q in range(0, rows // SUB, 2):
                r = slice(q * SUB, (q + 2) * SUB)
                w = pert[m, e * per + l, r].astype(jnp.float32) * g[e * per + l, r]
                place(lhs, s * rows + q * SUB, w, *pair(left[mine], right[mine], q * DEPTH))

    def margins(t):
        each = LANES // (2 * DEPTH)
        for a in range(sides):
            def fill():
                left, right = (root(rcor[a, b, t], 4) * (1.0 / CORNER) for b in range(2))
                for s in range(SUB):
                    j, i = s // each, s % each
                    mine = slice(j * SUB, (j + 1) * SUB)
                    w = [decode(rlat.at[a, t], (k * SUB + s) * DEPTH, DEPTH) for k in range(cols // LANES)]
                    place(lhm, (s * sides + a) * DEPTH, jnp.concatenate(w, 1),
                          *pair(left[mine], right[mine], i * 2 * DEPTH))

            if sides == 1:
                fill()
            else:
                pl.when(gets[a])(fill)

                @pl.when(jnp.logical_not(gets[a]))
                def _():
                    zero = jnp.zeros((DEPTH, 2 * LANES), jnp.bfloat16)
                    for s in range(SUB):
                        for k in range(3):
                            at = (s * sides + a) * DEPTH
                            lhm[k, at : at + DEPTH] = zero

    def damping(l):
        k1 = jnp.full((SUB, LANES), kappa[l], jnp.float32)
        scale = 1.0 / (1.0 + 4.0 * k1)
        tiles = []
        for i in range(0, full, SUB):
            n = k1 * eigen[kind, i : i + SUB]
            p = jnp.ones_like(n)
            for _ in range(SWEEPS):
                p = scale * (1.0 + n * p)
            for _ in range((2 * PASSES).bit_length() - 1):
                p = p * p
            tiles.append(p)
        return jnp.concatenate(tiles, 0)

    def dot(x, y):
        return jnp.dot(x, y, preferred_element_type=jnp.float32)

    def columns(t, source, first, count):
        for k in range(3):
            c = dot(source[k], into_c[k])
            for s in range(SUB):
                z = c[s * count : (s + 1) * count]
                high, low = split(z[:, :LANES] + z[:, LANES:])
                lanes = slice(k * LANES, (k + 1) * LANES)
                mid[t, s, first : first + count, lanes] = high
                mid[t, s, full + first : full + first + count, lanes] = low

    def start(t):
        for b in range(2):
            lon_copy(t, b).wait_recv()
        windows(t)
        columns(t, lhs, 0, rows)

    def transform(t):
        e = group(t)
        if sides:
            columns(t, lhm, rows, sides * DEPTH)
        for l in range(per):
            p = damping(e * per + l)
            p = jnp.concatenate([p, p, p], 1)
            batch = [m * per + l for m in range(members)]
            first = jnp.concatenate([mid[t, s, :full] for s in batch], 1)
            second = jnp.concatenate([mid[t, s, full:] for s in batch], 1)
            c = dot(into_r[kind], jnp.concatenate([first, first, second], 0))
            first, second = split(c * jnp.concatenate([p] * members, 1))
            c = dot(back_r[kind], jnp.concatenate([first, first, second], 0))
            first, second = split(c)
            for i, s in enumerate(batch):
                for k in range(3):
                    lanes = slice((3 * i + k) * LANES, (3 * i + k + 1) * LANES)
                    rhs[k, s * rows : (s + 1) * rows, :LANES] = first[:, lanes]
                    rhs[k, s * rows : (s + 1) * rows, LANES:] = second[:, lanes]

    def work(t, carry):
        e = group(t)
        start(t)
        for a in range(2):
            @pl.when(gets[a])
            def _():
                lat_copy(t, a).wait_recv()
                for b in range(2):
                    cor_copy(t, a, b).wait_recv()
        margins(t)
        transform(t)
        lane2 = lax.broadcasted_iota(jnp.int32, (rows, LANES), 1)
        sums = [[0.0, 0.0] for _ in range(per)]
        y = [dot(rhs[k], back_c[k]) for k in range(3)]
        y = [v[:, :LANES] + v[:, LANES:] for v in y]
        for l in range(per):
            for m in range(members):
                s = m * per + l
                r = slice(s * rows, (s + 1) * rows)
                v = pert[m, e * per + l].astype(jnp.float32)
                low = jnp.where(lane2 < LANES - 2 * DEPTH, y[0][r], y[1][r])
                high = jnp.where(lane2 < 2 * DEPTH, y[1][r], y[2][r])
                sums[l][0] = sums[l][0] + v[:, :LANES] * low
                sums[l][1] = sums[l][1] + v[:, LANES:] * high
            tap = taper[e * per + l] * (1.0 / (members * n_mem - 1))
            total = jnp.concatenate(sums[l], 1) * tap
            own[l] = total

        @pl.when(t < n_mem - 1)
        def _():
            @pl.when(jnp.logical_and(t == 0, mem < n_mem - 1))
            def _():
                pl.semaphore_wait(ready, n_mem - 1 - mem)

            encode(part.at[t], own[...].reshape(per * rows, cols))
            part_copy(t).start()

        return carry

    lax.fori_loop(0, n_mem, work, 0)
    for i in range(n_mem - 1):
        part_come(i).wait_recv()
    for k in range(cols // LANES):
        lanes = slice(k * LANES, (k + 1) * LANES)
        total = own[:, :, lanes].reshape(per * rows, LANES)
        for i in range(n_mem - 1):
            total = total + decode(rpart.at[i], k * per * rows, per * rows)
        out[:, :, lanes] = total.reshape(per, rows, LANES)

    def drain(t, carry):
        for b in range(2):
            lon_copy(t, b).wait_send()
        for a in range(2):
            @pl.when(sends[a])
            def _():
                lat_copy(t, a).wait_send()
                for b in range(2):
                    cor_copy(t, a, b).wait_send()
        return carry

    lax.fori_loop(0, n_mem, drain, 0)
    for t in range(n_mem - 1):
        part_copy(t).wait_send()


def local(sizes, perturbations, increment, taper_norm, kappa):
    n_mem, n_lat, n_lon = sizes
    members, levels, rows, cols = perturbations.shape
    per = levels // n_mem
    assert members * per == SUB and cols == 2 * LANES and rows * DEPTH == SUB * LANES
    f32, bf16 = jnp.float32, jnp.bfloat16
    sides = min(n_lat - 1, 2)
    full = rows + sides * DEPTH
    tiles = SUB * 2 * DEPTH // LANES
    into_c, back_c, eig = column_tables()
    tables = (into_c, back_c) + row_tables(rows, sides, eig)
    arrays = (perturbations, increment, taper_norm, *map(jnp.asarray, tables))
    dma = pltpu.SemaphoreType.DMA
    vmem = pl.BlockSpec(memory_space=pltpu.VMEM)
    return pl.pallas_call(
        functools.partial(kernel, sizes),
        out_shape=pltpu.VMEM((per, rows, cols), f32),
        in_specs=[pl.BlockSpec(memory_space=pltpu.SMEM)] + [pl.BlockSpec(memory_space=pl.ANY)] * len(arrays),
        out_specs=vmem,
        scratch_shapes=[pltpu.VMEM(array.shape, array.dtype) for array in arrays] + [
            dma((3, n_mem)), dma((5,)), pltpu.SemaphoreType.REGULAR,
            pltpu.VMEM((levels, rows, cols), f32),
            pltpu.VMEM((2, n_mem, 2 * SUB + SUB * SUB, LANES), bf16),
            pltpu.VMEM((2, n_mem, 2 * SUB + SUB * SUB, LANES), bf16),
            pltpu.VMEM((2, 2, n_mem, tiles * SUB, LANES), bf16),
            pltpu.VMEM((2, 2, n_mem, tiles * SUB, LANES), bf16),
            pltpu.VMEM((2, n_mem, 2 * SUB + SUB * DEPTH * cols // LANES, LANES), bf16),
            pltpu.VMEM((2, n_mem, 2 * SUB + SUB * DEPTH * cols // LANES, LANES), bf16),
            pltpu.VMEM((3, SUB * rows, 2 * LANES), bf16),
            pltpu.VMEM((3, SUB * max(sides, 1) * DEPTH, 2 * LANES), bf16),
            pltpu.VMEM((n_mem, SUB, 2 * full, 3 * LANES), bf16),
            pltpu.VMEM((3, SUB * rows, 2 * LANES), jnp.bfloat16),
            pltpu.VMEM((per, rows, cols), f32),
            pltpu.VMEM((n_mem - 1, 2 * SUB + per * rows * cols // LANES, LANES), bf16),
            pltpu.VMEM((n_mem - 1, 2 * SUB + per * rows * cols // LANES, LANES), bf16),
            dma((2, n_mem)), dma((2, n_mem)),
            dma((2, n_mem)), dma((2, n_mem)),
            dma((2, 2, n_mem)), dma((2, 2, n_mem)),
            dma((n_mem - 1,)), dma((n_mem - 1,)),
        ],
        compiler_params=pltpu.CompilerParams(collective_id=0, has_side_effects=True),
    )(kappa, *arrays)


def solution(mesh):
    sizes = tuple(mesh.shape[name] for name in ("mem", "lat", "lon"))
    return jax.shard_map(
        functools.partial(local, sizes),
        mesh=mesh,
        in_specs=(P("mem", None, "lat", "lon"), P(None, "lat", "lon"), P(None, "lat", "lon"), P()),
        out_specs=P("mem", "lat", "lon"),
        check_vma=False,
    )
```

```python
import functools

import jax
import jax.numpy as jnp
import numpy as np
from jax import lax
from jax.experimental import pallas as pl
from jax.experimental.pallas import tpu as pltpu
from jax.sharding import PartitionSpec as P

PASSES = 4
SWEEPS = 2
DEPTH = 2 * PASSES * SWEEPS
SUB = 8
LANES = 128
MESH = pl.DeviceIdType.MESH
ROOT = 4
PEAK = 2.0 ** (126 / 2**ROOT)
CORNER = 2.0 ** (126 / 4) / 6.0**3


def roll(value, shift):
    shift = lax.rem(shift, LANES) if isinstance(shift, jax.Array) else shift % LANES
    return value if isinstance(shift, int) and shift == 0 else pltpu.roll(value, shift, value.ndim - 1)


def halves(matrix):
    high = np.asarray(matrix, np.float64).astype(jnp.bfloat16)
    return high, (matrix - high.astype(np.float64)).astype(jnp.bfloat16)


def sine(n):
    order = np.arange(1, n + 1)
    basis = np.sqrt(2.0 / (n + 1)) * np.sin(np.pi * np.outer(order, order) / (n + 1))
    return basis, 2.0 * np.cos(np.pi * order / (n + 1))


def column_tables():
    basis, own = sine(LANES)
    lanes = np.arange(LANES)
    into, back = [], []
    for shift in (DEPTH, LANES // 2, -DEPTH):
        high, low = halves(basis[(lanes + shift) % LANES])
        into.append(np.block([[high, low], [high, low]]))
        back.append(np.block([[high.T, low.T], [high.T, low.T]]))
    return np.stack(into), np.stack(back), own


def row_tables(rows, sides, columns):
    full = rows + sides * DEPTH
    kinds = [[], [0, 1], [0, 1, 2]][sides] or [None]
    into, back, own = [], [], []
    for kind in kinds:
        above = sides == 2 and kind > 0 or sides == 1 and kind == 1
        below = sides == 2 and kind < 2 or sides == 1 and kind == 0
        start = DEPTH if above else 0
        size = rows + start + (DEPTH if below else 0)
        basis, eig = sine(size)
        spots = [np.arange(start, start + rows)]
        for side, there in enumerate((above, below)):
            first = 0 if side == 0 else start + rows
            if there:
                spots.append(np.arange(first, first + DEPTH))
            elif sides == 2:
                spots.append(np.full(DEPTH, -1))
        spots = np.concatenate(spots)
        table = np.zeros((full, full))
        table[:size] = np.where(spots < 0, 0.0, basis[:, spots])
        high, low = halves(table)
        into.append(np.concatenate([high, low, high], 1))
        high, low = halves(table.T[:rows])
        back.append(np.concatenate([high, low, high], 1))
        sums = np.zeros((full, LANES))
        sums[:size] = eig[:, None] + columns
        own.append(sums.astype(np.float32))
    return np.stack(into), np.stack(back), np.stack(own)


def split(value):
    high = value.astype(jnp.bfloat16)
    return high, (value - high.astype(jnp.float32)).astype(jnp.bfloat16)


def top(value):
    tiles = [
        jnp.abs(value[i : i + SUB, j : j + LANES])
        for i in range(0, value.shape[0], SUB)
        for j in range(0, value.shape[1], LANES)
    ]
    while len(tiles) > 1:
        tiles = [jnp.maximum(*tiles[i : i + 2]) if tiles[i + 1 :] else tiles[i] for i in range(0, len(tiles), 2)]
    return tiles[0]


def spread(tile, like):
    tile = jnp.concatenate([tile] * (like.shape[1] // LANES), 1)
    return jnp.concatenate([tile] * (like.shape[0] // SUB), 0)


def power(value, squares):
    negative = value < 0.0
    for _ in range(squares):
        value = value * value
    return jnp.where(negative, -value, value).astype(jnp.bfloat16)


def root(coded, order):
    coded = coded.astype(jnp.float32)
    value = jnp.exp2(jnp.log2(jnp.abs(coded)) * (1.0 / order))
    return jnp.where(coded < 0.0, -value, value)


def encode(message, value):
    scale = jnp.maximum(top(value), 1e-30).astype(jnp.bfloat16)
    message[: 2 * SUB] = jnp.concatenate([scale, scale], 0)
    coded = power(value * spread(PEAK / scale.astype(jnp.float32), value), ROOT)
    for i in range(value.shape[1] // LANES):
        message[pl.ds(2 * SUB + i * value.shape[0], value.shape[0])] = coded[:, i * LANES : (i + 1) * LANES]


def decode(message, start, count):
    scale = message[: 2 * SUB].astype(jnp.float32)[:SUB] * (1.0 / PEAK)
    value = root(message[pl.ds(2 * SUB + start, count)], 2**ROOT)
    return value * spread(scale, value)


def kernel(
    sizes, kappa, pert_h, inc_h, taper_h, into_c_h, back_c_h, into_r_h, back_r_h, eigen_h, out,
    pert, inc, taper, into_c, back_c, into_r, back_r, eigen, load, load_c, ready, g, pack, rlon, cpack, rcor, epack, rlat, lhs, lhm, mid, rhs, own, part, rpart,
    lon_send, lon_recv, lat_send, lat_recv, cor_send, cor_recv, part_send, part_recv,
):
    n_mem, n_lat, n_lon = sizes
    mem, lat, lon = lax.axis_index("mem"), lax.axis_index("lat"), lax.axis_index("lon")
    members, levels, rows, cols = pert.shape
    per = levels // n_mem
    sides = min(n_lat - 1, 2)
    full = rows + sides * DEPTH
    kind = jnp.where(lat == 0, 0, jnp.where(lat == n_lat - 1, sides, 1)) if sides else 0
    lane = lax.broadcasted_iota(jnp.int32, (SUB, LANES), 1)
    lon_to = [lax.rem(lon + 1, n_lon), lax.rem(lon + n_lon - 1, n_lon)]
    if sides == 1:
        lat_to, sends, gets, edge = [1 - lat], [None], [None], [jnp.where(lat == 0, rows - DEPTH, 0)]
    else:
        lat_to = [lat + 1, lat - 1][:sides]
        sends = [lat < n_lat - 1, lat > 0][:sides]
        gets = [lat > 0, lat < n_lat - 1][:sides]
        edge = [rows - DEPTH, 0]

    def where_(test):
        return pl.when(test) if test is not None else lambda body: body()

    def group(t):
        near = jnp.minimum(mem, n_mem - 1 - mem)
        ends = jnp.where(lax.rem(t, 2) == 0, lax.div(t, 2), n_mem - 1 - lax.div(t, 2))
        rest = jnp.where(2 * mem >= n_mem, t - near, n_mem - 1 - t + near)
        inner = jnp.logical_and(t > 0, t < n_mem - 1)
        e = jnp.where(t < 2 * near, ends, rest)
        return jnp.where(jnp.logical_and(mem == n_mem - 1, inner), n_mem - 1 - t, e)

    def spot(here, there):
        return lax.rem(here - there + n_mem - 1, n_mem)

    def remote(src, dst, send, recv, **where):
        return pltpu.make_async_remote_copy(
            src_ref=src, dst_ref=dst, send_sem=send, recv_sem=recv,
            device_id=where, device_id_type=MESH,
        )

    def lon_copy(t, b):
        return remote(pack.at[b, t], rlon.at[b, t], lon_send.at[b, t], lon_recv.at[b, t],
                      mem=mem, lat=lat, lon=lon_to[b])

    def cor_copy(t, a, b):
        return remote(cpack.at[a, b, t], rcor.at[a, b, t], cor_send.at[a, b, t],
                      cor_recv.at[a, b, t], mem=mem, lat=lat_to[a], lon=lon_to[b])

    def lat_copy(t, a):
        return remote(epack.at[a, t], rlat.at[a, t], lat_send.at[a, t], lat_recv.at[a, t],
                      mem=mem, lat=lat_to[a], lon=lon)

    def part_copy(t):
        e = group(t)
        i = spot(mem, e)
        return remote(part.at[t], rpart.at[i], part_send.at[t], part_recv.at[i],
                      mem=e, lat=lat, lon=lon)

    def part_come(i):
        return remote(part.at[i], rpart.at[i], part_send.at[i], part_recv.at[i],
                      mem=lax.rem(mem + 1, n_mem), lat=lat, lon=lon)

    def pieces(t):
        mine = pl.ds(group(t) * per, per)
        return [
            pltpu.make_async_copy(source, target, load.at[i, t])
            for i, (source, target) in enumerate((
                (inc_h.at[mine], inc.at[mine]), (taper_h.at[mine], taper.at[mine]),
                (pert_h.at[:, mine], pert.at[:, mine]),
            ))
        ]

    tables = [
        pltpu.make_async_copy(source, target, load_c.at[i])
        for i, (source, target) in enumerate((
            (into_c_h, into_c), (into_r_h, into_r), (eigen_h, eigen), (back_r_h, back_r), (back_c_h, back_c),
        ))
    ]
    for copy in pieces(0) + tables[:1] + pieces(1) + tables[1:]:
        copy.start()
    for t in range(2, n_mem):
        for copy in pieces(t):
            copy.start()

    barrier = pltpu.get_barrier_semaphore()

    def greet(**where):
        pl.semaphore_signal(barrier, inc=1, device_id=where, device_id_type=MESH)

    for b in range(2):
        greet(mem=mem, lat=lat, lon=lon_to[b])
    for d in range(1, n_mem):
        @pl.when(mem + d < n_mem)
        def _():
            greet(mem=mem + d, lat=lat, lon=lon)
    for a in range(sides):
        @where_(sends[a])
        def _():
            greet(mem=mem, lat=lat_to[a], lon=lon)
            for b in range(2):
                greet(mem=mem, lat=lat_to[a], lon=lon_to[b])

    beside = sum(1 if s is None else jnp.where(s, 1, 0) for s in sends)
    pl.semaphore_wait(barrier, 2 + mem + 3 * beside)
    for d in range(1, n_mem):
        @pl.when(mem >= d)
        def _():
            pl.semaphore_signal(ready, inc=1, device_id=dict(mem=mem - d, lat=lat, lon=lon), device_id_type=MESH)

    def send_group(t, carry):
        e = group(t)
        for copy in pieces(t):
            copy.wait()
        mine = pl.ds(e * per, per)
        g[mine] = taper[mine] * inc[mine]
        for a in range(sides):
            @where_(sends[a])
            def _():
                r = pl.ds(edge[a], DEPTH)
                w = [
                    pert[s // per, e * per + s % per, r, :].astype(jnp.float32) * g[e * per + s % per, r, :]
                    for s in range(SUB)
                ]
                encode(epack.at[a, t], jnp.concatenate(w, 0))
                lat_copy(t, a).start()

        each = LANES // (2 * DEPTH)
        corners = [[[None] * (SUB // each) for _ in range(2)] for _ in range(sides)]
        edges = [[], []]
        for s in range(SUB):
            m, l = s // per, s % per
            j, i = s // each, s % each
            for b, column in enumerate((cols - LANES, 0)):
                source = LANES - DEPTH if b == 0 else 0
                w = pert[m, e * per + l, :, pl.ds(column, LANES)].astype(jnp.float32)
                w = w * g[e * per + l, :, pl.ds(column, LANES)]
                acc = None
                for q in range(rows // SUB):
                    v = roll(w[q * SUB : (q + 1) * SUB], q * DEPTH - source)
                    acc = v if acc is None else jnp.where(lane >= q * DEPTH, v, acc)
                edges[b].append(acc)
                for a in range(sides):
                    v = roll(acc, LANES + i * 2 * DEPTH - edge[a] // SUB * DEPTH)
                    old = corners[a][b][j]
                    corners[a][b][j] = v if old is None else jnp.where(lane >= i * 2 * DEPTH, v, old)
        for b in range(2):
            encode(pack.at[b, t], jnp.concatenate(edges[b], 0))
            for a in range(sides):
                cpack[a, b, t] = power(jnp.concatenate(corners[a][b], 0) * CORNER, 2)
        for b in range(2):
            lon_copy(t, b).start()
        for a in range(sides):
            @where_(sends[a])
            def _():
                for b in range(2):
                    cor_copy(t, a, b).start()
        return carry

    lax.fori_loop(0, n_mem, send_group, 0)
    for copy in tables:
        copy.wait()

    lane1 = lax.broadcasted_iota(jnp.int32, (2 * SUB, LANES), 1)

    def place(lhs, at, x, low, high):
        x0, x1 = x[:, :LANES], x[:, LANES:]
        views = (
            jnp.where(lane1 < LANES - DEPTH, x0, low),
            jnp.where(lane1 < LANES // 2, x1, x0),
            jnp.where(lane1 < DEPTH, high, x1),
        )
        for k, view in enumerate(views):
            first, second = split(view)
            lhs[k, at : at + 2 * SUB, :LANES] = first
            lhs[k, at : at + 2 * SUB, LANES:] = second

    def pair(left, right, at):
        low = [roll(left, LANES - DEPTH - at - h * DEPTH) for h in range(2)]
        high = [roll(right, -at - h * DEPTH) for h in range(2)]
        return jnp.concatenate(low, 0), jnp.concatenate(high, 0)

    def windows(t):
        e = group(t)
        left, right = (decode(rlon.at[b, t], 0, SUB * SUB) for b in range(2))
        for s in range(SUB):
            m, l = s // per, s % per
            mine = slice(s * SUB, (s + 1) * SUB)
            for q in range(0, rows // SUB, 2):
                r = slice(q * SUB, (q + 2) * SUB)
                w = pert[m, e * per + l, r].astype(jnp.float32) * g[e * per + l, r]
                place(lhs, s * rows + q * SUB, w, *pair(left[mine], right[mine], q * DEPTH))

    def margins(t):
        each = LANES // (2 * DEPTH)
        for a in range(sides):
            def fill():
                left, right = (root(rcor[a, b, t], 4) * (1.0 / CORNER) for b in range(2))
                for s in range(SUB):
                    j, i = s // each, s % each
                    mine = slice(j * SUB, (j + 1) * SUB)
                    w = [decode(rlat.at[a, t], (k * SUB + s) * DEPTH, DEPTH) for k in range(cols // LANES)]
                    place(lhm, (s * sides + a) * DEPTH, jnp.concatenate(w, 1),
                          *pair(left[mine], right[mine], i * 2 * DEPTH))

            where_(gets[a])(fill)
            if gets[a] is not None:
                @pl.when(jnp.logical_not(gets[a]))
                def _():
                    zero = jnp.zeros((DEPTH, 2 * LANES), jnp.bfloat16)
                    for s in range(SUB):
                        for k in range(3):
                            at = (s * sides + a) * DEPTH
                            lhm[k, at : at + DEPTH] = zero

    def damping(l):
        k1 = jnp.full((SUB, LANES), kappa[l], jnp.float32)
        scale = 1.0 / (1.0 + 4.0 * k1)
        tiles = []
        for i in range(0, full, SUB):
            n = k1 * eigen[kind, i : i + SUB]
            p = jnp.ones_like(n)
            for _ in range(SWEEPS):
                p = scale * (1.0 + n * p)
            for _ in range((2 * PASSES).bit_length() - 1):
                p = p * p
            tiles.append(p)
        return jnp.concatenate(tiles, 0)

    def dot(x, y):
        return jnp.dot(x, y, preferred_element_type=jnp.float32)

    def columns(t, source, first, count):
        for k in range(3):
            c = dot(source[k], into_c[k])
            for s in range(SUB):
                z = c[s * count : (s + 1) * count]
                high, low = split(z[:, :LANES] + z[:, LANES:])
                lanes = slice(k * LANES, (k + 1) * LANES)
                mid[t, s, first : first + count, lanes] = high
                mid[t, s, full + first : full + first + count, lanes] = low

    def start(t):
        for b in range(2):
            lon_copy(t, b).wait_recv()
        windows(t)
        columns(t, lhs, 0, rows)

    def transform(t):
        e = group(t)
        if sides:
            columns(t, lhm, rows, sides * DEPTH)
        for l in range(per):
            p = damping(e * per + l)
            p = jnp.concatenate([p, p, p], 1)
            batch = [m * per + l for m in range(members)]
            first = jnp.concatenate([mid[t, s, :full] for s in batch], 1)
            second = jnp.concatenate([mid[t, s, full:] for s in batch], 1)
            c = dot(into_r[kind], jnp.concatenate([first, first, second], 0))
            first, second = split(c * jnp.concatenate([p] * members, 1))
            c = dot(back_r[kind], jnp.concatenate([first, first, second], 0))
            first, second = split(c)
            for i, s in enumerate(batch):
                for k in range(3):
                    lanes = slice((3 * i + k) * LANES, (3 * i + k + 1) * LANES)
                    rhs[k, s * rows : (s + 1) * rows, :LANES] = first[:, lanes]
                    rhs[k, s * rows : (s + 1) * rows, LANES:] = second[:, lanes]

    def work(t, carry):
        e = group(t)
        start(t)
        for a in range(sides):
            @where_(gets[a])
            def _():
                lat_copy(t, a).wait_recv()
                for b in range(2):
                    cor_copy(t, a, b).wait_recv()
        margins(t)
        transform(t)
        lane2 = lax.broadcasted_iota(jnp.int32, (rows, LANES), 1)
        sums = [[0.0, 0.0] for _ in range(per)]
        y = [dot(rhs[k], back_c[k]) for k in range(3)]
        y = [v[:, :LANES] + v[:, LANES:] for v in y]
        for l in range(per):
            for m in range(members):
                s = m * per + l
                r = slice(s * rows, (s + 1) * rows)
                v = pert[m, e * per + l].astype(jnp.float32)
                low = jnp.where(lane2 < LANES - 2 * DEPTH, y[0][r], y[1][r])
                high = jnp.where(lane2 < 2 * DEPTH, y[1][r], y[2][r])
                sums[l][0] = sums[l][0] + v[:, :LANES] * low
                sums[l][1] = sums[l][1] + v[:, LANES:] * high
            tap = taper[e * per + l] * (1.0 / (members * n_mem - 1))
            total = jnp.concatenate(sums[l], 1) * tap
            own[l] = total

        @pl.when(t < n_mem - 1)
        def _():
            @pl.when(jnp.logical_and(t == 0, mem < n_mem - 1))
            def _():
                pl.semaphore_wait(ready, n_mem - 1 - mem)

            encode(part.at[t], own[...].reshape(per * rows, cols))
            part_copy(t).start()

        return carry

    lax.fori_loop(0, n_mem, work, 0)
    for i in range(n_mem - 1):
        part_come(i).wait_recv()
    for k in range(cols // LANES):
        lanes = slice(k * LANES, (k + 1) * LANES)
        total = own[:, :, lanes].reshape(per * rows, LANES)
        for i in range(n_mem - 1):
            total = total + decode(rpart.at[i], k * per * rows, per * rows)
        out[:, :, lanes] = total.reshape(per, rows, LANES)

    def drain(t, carry):
        for b in range(2):
            lon_copy(t, b).wait_send()
        for a in range(sides):
            @where_(sends[a])
            def _():
                lat_copy(t, a).wait_send()
                for b in range(2):
                    cor_copy(t, a, b).wait_send()
        return carry

    lax.fori_loop(0, n_mem, drain, 0)
    for t in range(n_mem - 1):
        part_copy(t).wait_send()


def local(sizes, perturbations, increment, taper_norm, kappa):
    n_mem, n_lat, n_lon = sizes
    members, levels, rows, cols = perturbations.shape
    per = levels // n_mem
    assert members * per == SUB and cols == 2 * LANES and rows * DEPTH == SUB * LANES
    f32, bf16 = jnp.float32, jnp.bfloat16
    sides = min(n_lat - 1, 2)
    full = rows + sides * DEPTH
    tiles = SUB * 2 * DEPTH // LANES
    into_c, back_c, eig = column_tables()
    tables = (into_c, back_c) + row_tables(rows, sides, eig)
    arrays = (perturbations, increment, taper_norm, *map(jnp.asarray, tables))
    dma = pltpu.SemaphoreType.DMA
    vmem = pl.BlockSpec(memory_space=pltpu.VMEM)
    return pl.pallas_call(
        functools.partial(kernel, sizes),
        out_shape=pltpu.VMEM((per, rows, cols), f32),
        in_specs=[pl.BlockSpec(memory_space=pltpu.SMEM)] + [pl.BlockSpec(memory_space=pl.ANY)] * len(arrays),
        out_specs=vmem,
        scratch_shapes=[pltpu.VMEM(array.shape, array.dtype) for array in arrays] + [
            dma((3, n_mem)), dma((5,)), pltpu.SemaphoreType.REGULAR,
            pltpu.VMEM((levels, rows, cols), f32),
            pltpu.VMEM((2, n_mem, 2 * SUB + SUB * SUB, LANES), bf16),
            pltpu.VMEM((2, n_mem, 2 * SUB + SUB * SUB, LANES), bf16),
            pltpu.VMEM((2, 2, n_mem, tiles * SUB, LANES), bf16),
            pltpu.VMEM((2, 2, n_mem, tiles * SUB, LANES), bf16),
            pltpu.VMEM((2, n_mem, 2 * SUB + SUB * DEPTH * cols // LANES, LANES), bf16),
            pltpu.VMEM((2, n_mem, 2 * SUB + SUB * DEPTH * cols // LANES, LANES), bf16),
            pltpu.VMEM((3, SUB * rows, 2 * LANES), bf16),
            pltpu.VMEM((3, SUB * max(sides, 1) * DEPTH, 2 * LANES), bf16),
            pltpu.VMEM((n_mem, SUB, 2 * full, 3 * LANES), bf16),
            pltpu.VMEM((3, SUB * rows, 2 * LANES), jnp.bfloat16),
            pltpu.VMEM((per, rows, cols), f32),
            pltpu.VMEM((n_mem - 1, 2 * SUB + per * rows * cols // LANES, LANES), bf16),
            pltpu.VMEM((n_mem - 1, 2 * SUB + per * rows * cols // LANES, LANES), bf16),
            dma((2, n_mem)), dma((2, n_mem)),
            dma((2, n_mem)), dma((2, n_mem)),
            dma((2, 2, n_mem)), dma((2, 2, n_mem)),
            dma((n_mem - 1,)), dma((n_mem - 1,)),
        ],
        compiler_params=pltpu.CompilerParams(collective_id=0, has_side_effects=True),
    )(kappa, *arrays)


def solution(mesh):
    sizes = tuple(mesh.shape[name] for name in ("mem", "lat", "lon"))
    return jax.shard_map(
        functools.partial(local, sizes),
        mesh=mesh,
        in_specs=(P("mem", None, "lat", "lon"), P(None, "lat", "lon"), P(None, "lat", "lon"), P()),
        out_specs=P("mem", "lat", "lon"),
        check_vma=False,
    )
```

```python
import functools

import jax
import jax.numpy as jnp
import numpy as np
from jax import lax
from jax.experimental import pallas as pl
from jax.experimental.pallas import tpu as pltpu
from jax.sharding import PartitionSpec as P

PASSES = 4
SWEEPS = 2
DEPTH = 2 * PASSES * SWEEPS
SUB = 8
LANES = 128
MESH = pl.DeviceIdType.MESH
ROOT = 4
PEAK = 2.0 ** (126 / 2**ROOT)
CORNER = 2.0 ** (126 / 4) / 6.0**3


def roll(value, shift):
    shift = lax.rem(shift, LANES) if isinstance(shift, jax.Array) else shift % LANES
    return value if isinstance(shift, int) and shift == 0 else pltpu.roll(value, shift, value.ndim - 1)


def halves(matrix):
    high = np.asarray(matrix, np.float64).astype(jnp.bfloat16)
    return high, (matrix - high.astype(np.float64)).astype(jnp.bfloat16)


def sine(n):
    order = np.arange(1, n + 1)
    basis = np.sqrt(2.0 / (n + 1)) * np.sin(np.pi * np.outer(order, order) / (n + 1))
    return basis, 2.0 * np.cos(np.pi * order / (n + 1))


def column_tables():
    basis, own = sine(LANES)
    lanes = np.arange(LANES)
    into, back = [], []
    for shift in (DEPTH, LANES // 2, -DEPTH):
        high, low = halves(basis[(lanes + shift) % LANES])
        into.append(np.block([[high, low], [high, low]]))
        back.append(np.block([[high.T, low.T], [high.T, low.T]]))
    return np.stack(into), np.stack(back), own


def row_tables(rows, sides, columns):
    full = rows + sides * DEPTH
    kinds = [[], [0, 1], [0, 1, 2]][sides] or [None]
    into, back, own = [], [], []
    for kind in kinds:
        above = sides == 2 and kind > 0 or sides == 1 and kind == 1
        below = sides == 2 and kind < 2 or sides == 1 and kind == 0
        start = DEPTH if above else 0
        size = rows + start + (DEPTH if below else 0)
        basis, eig = sine(size)
        spots = [np.arange(start, start + rows)]
        for side, there in enumerate((above, below)):
            first = 0 if side == 0 else start + rows
            if there:
                spots.append(np.arange(first, first + DEPTH))
            elif sides == 2:
                spots.append(np.full(DEPTH, -1))
        spots = np.concatenate(spots)
        table = np.zeros((full, full))
        table[:size] = np.where(spots < 0, 0.0, basis[:, spots])
        high, low = halves(table)
        into.append(np.concatenate([high, low, high], 1))
        high, low = halves(table.T[:rows])
        back.append(np.concatenate([high, low, high], 1))
        sums = np.zeros((full, LANES))
        sums[:size] = eig[:, None] + columns
        own.append(sums.astype(np.float32))
    return np.stack(into), np.stack(back), np.stack(own)


def split(value):
    high = value.astype(jnp.bfloat16)
    return high, (value - high.astype(jnp.float32)).astype(jnp.bfloat16)


def top(value):
    tiles = [
        jnp.abs(value[i : i + SUB, j : j + LANES])
        for i in range(0, value.shape[0], SUB)
        for j in range(0, value.shape[1], LANES)
    ]
    while len(tiles) > 1:
        tiles = [jnp.maximum(*tiles[i : i + 2]) if tiles[i + 1 :] else tiles[i] for i in range(0, len(tiles), 2)]
    return tiles[0]


def spread(tile, like):
    tile = jnp.concatenate([tile] * (like.shape[1] // LANES), 1)
    return jnp.concatenate([tile] * (like.shape[0] // SUB), 0)


def power(value, squares):
    negative = value < 0.0
    for _ in range(squares):
        value = value * value
    return jnp.where(negative, -value, value).astype(jnp.bfloat16)


def root(coded, order):
    coded = coded.astype(jnp.float32)
    value = jnp.exp2(jnp.log2(jnp.abs(coded)) * (1.0 / order))
    return jnp.where(coded < 0.0, -value, value)


def encode(message, value):
    scale = jnp.maximum(top(value), 1e-30).astype(jnp.bfloat16)
    message[: 2 * SUB] = jnp.concatenate([scale, scale], 0)
    coded = power(value * spread(PEAK / scale.astype(jnp.float32), value), ROOT)
    for i in range(value.shape[1] // LANES):
        message[pl.ds(2 * SUB + i * value.shape[0], value.shape[0])] = coded[:, i * LANES : (i + 1) * LANES]


def decode(message, start, count):
    scale = message[: 2 * SUB].astype(jnp.float32)[:SUB] * (1.0 / PEAK)
    value = root(message[pl.ds(2 * SUB + start, count)], 2**ROOT)
    return value * spread(scale, value)


def kernel(
    sizes, kappa, pert_h, inc_h, taper_h, into_c_h, back_c_h, into_r_h, back_r_h, eigen_h, out,
    pert, inc, taper, into_c, back_c, into_r, back_r, eigen, load, load_c, ready, g, pack, rlon, cpack, rcor, epack, rlat, lhs, lhm, mid, rhs, own, part, rpart,
    lon_send, lon_recv, lat_send, lat_recv, cor_send, cor_recv, part_send, part_recv,
):
    n_mem, n_lat, n_lon = sizes
    mem, lat, lon = lax.axis_index("mem"), lax.axis_index("lat"), lax.axis_index("lon")
    members, levels, rows, cols = pert.shape
    per = levels // n_mem
    sides = min(n_lat - 1, 2)
    full = rows + sides * DEPTH
    kind = jnp.where(lat == 0, 0, jnp.where(lat == n_lat - 1, sides, 1)) if sides else 0
    lane = lax.broadcasted_iota(jnp.int32, (SUB, LANES), 1)
    lon_to = [lax.rem(lon + 1, n_lon), lax.rem(lon + n_lon - 1, n_lon)]
    if sides == 1:
        lat_to, sends, gets, edge = [1 - lat], [None], [None], [jnp.where(lat == 0, rows - DEPTH, 0)]
    else:
        lat_to = [lat + 1, lat - 1][:sides]
        sends = [lat < n_lat - 1, lat > 0][:sides]
        gets = [lat > 0, lat < n_lat - 1][:sides]
        edge = [rows - DEPTH, 0]

    def where_(test):
        return pl.when(test) if test is not None else lambda body: body()

    def group(t):
        e = jnp.where(t < mem, t, n_mem - 1 - t + mem)
        last = jnp.logical_and(mem == n_mem - 1, t > 0)
        return jnp.where(t == n_mem - 1, mem, jnp.where(last, n_mem - 1 - t, e))

    def spot(here, there):
        return lax.rem(here - there + n_mem - 1, n_mem)

    def remote(src, dst, send, recv, **where):
        return pltpu.make_async_remote_copy(
            src_ref=src, dst_ref=dst, send_sem=send, recv_sem=recv,
            device_id=where, device_id_type=MESH,
        )

    def lon_copy(t, b):
        return remote(pack.at[b, t], rlon.at[b, t], lon_send.at[b, t], lon_recv.at[b, t],
                      mem=mem, lat=lat, lon=lon_to[b])

    def cor_copy(t, a, b):
        return remote(cpack.at[a, b, t], rcor.at[a, b, t], cor_send.at[a, b, t],
                      cor_recv.at[a, b, t], mem=mem, lat=lat_to[a], lon=lon_to[b])

    def lat_copy(t, a):
        return remote(epack.at[a, t], rlat.at[a, t], lat_send.at[a, t], lat_recv.at[a, t],
                      mem=mem, lat=lat_to[a], lon=lon)

    def part_copy(t):
        e = group(t)
        i = spot(mem, e)
        return remote(part.at[t], rpart.at[i], part_send.at[t], part_recv.at[i],
                      mem=e, lat=lat, lon=lon)

    def part_come(i):
        return remote(part.at[i], rpart.at[i], part_send.at[i], part_recv.at[i],
                      mem=lax.rem(mem + 1, n_mem), lat=lat, lon=lon)

    def pieces(t):
        mine = pl.ds(group(t) * per, per)
        return [
            pltpu.make_async_copy(source, target, load.at[i, t])
            for i, (source, target) in enumerate((
                (inc_h.at[mine], inc.at[mine]), (taper_h.at[mine], taper.at[mine]),
                (pert_h.at[:, mine], pert.at[:, mine]),
            ))
        ]

    tables = [
        pltpu.make_async_copy(source, target, load_c.at[i])
        for i, (source, target) in enumerate((
            (into_c_h, into_c), (into_r_h, into_r), (eigen_h, eigen), (back_r_h, back_r), (back_c_h, back_c),
        ))
    ]
    for copy in pieces(0) + tables[:1] + pieces(1) + tables[1:]:
        copy.start()
    for t in range(2, n_mem):
        for copy in pieces(t):
            copy.start()

    barrier = pltpu.get_barrier_semaphore()

    def greet(**where):
        pl.semaphore_signal(barrier, inc=1, device_id=where, device_id_type=MESH)

    for b in range(2):
        greet(mem=mem, lat=lat, lon=lon_to[b])
    for d in range(1, n_mem):
        @pl.when(mem + d < n_mem)
        def _():
            greet(mem=mem + d, lat=lat, lon=lon)
    for a in range(sides):
        @where_(sends[a])
        def _():
            greet(mem=mem, lat=lat_to[a], lon=lon)
            for b in range(2):
                greet(mem=mem, lat=lat_to[a], lon=lon_to[b])

    beside = sum(1 if s is None else jnp.where(s, 1, 0) for s in sends)
    pl.semaphore_wait(barrier, 2 + mem + 3 * beside)
    for d in range(1, n_mem):
        @pl.when(mem >= d)
        def _():
            pl.semaphore_signal(ready, inc=1, device_id=dict(mem=mem - d, lat=lat, lon=lon), device_id_type=MESH)

    def send_group(t, carry):
        e = group(t)
        for copy in pieces(t):
            copy.wait()
        mine = pl.ds(e * per, per)
        g[mine] = taper[mine] * inc[mine]
        for a in range(sides):
            @where_(sends[a])
            def _():
                r = pl.ds(edge[a], DEPTH)
                w = [
                    pert[s // per, e * per + s % per, r, :].astype(jnp.float32) * g[e * per + s % per, r, :]
                    for s in range(SUB)
                ]
                encode(epack.at[a, t], jnp.concatenate(w, 0))
                lat_copy(t, a).start()

        each = LANES // (2 * DEPTH)
        corners = [[[None] * (SUB // each) for _ in range(2)] for _ in range(sides)]
        edges = [[], []]
        for s in range(SUB):
            m, l = s // per, s % per
            j, i = s // each, s % each
            for b, column in enumerate((cols - LANES, 0)):
                source = LANES - DEPTH if b == 0 else 0
                w = pert[m, e * per + l, :, pl.ds(column, LANES)].astype(jnp.float32)
                w = w * g[e * per + l, :, pl.ds(column, LANES)]
                acc = None
                for q in range(rows // SUB):
                    v = roll(w[q * SUB : (q + 1) * SUB], q * DEPTH - source)
                    acc = v if acc is None else jnp.where(lane >= q * DEPTH, v, acc)
                edges[b].append(acc)
                for a in range(sides):
                    v = roll(acc, LANES + i * 2 * DEPTH - edge[a] // SUB * DEPTH)
                    old = corners[a][b][j]
                    corners[a][b][j] = v if old is None else jnp.where(lane >= i * 2 * DEPTH, v, old)
        for b in range(2):
            encode(pack.at[b, t], jnp.concatenate(edges[b], 0))
            for a in range(sides):
                cpack[a, b, t] = power(jnp.concatenate(corners[a][b], 0) * CORNER, 2)
        for b in range(2):
            lon_copy(t, b).start()
        for a in range(sides):
            @where_(sends[a])
            def _():
                for b in range(2):
                    cor_copy(t, a, b).start()
        return carry

    lax.fori_loop(0, n_mem, send_group, 0)
    for copy in tables:
        copy.wait()

    lane1 = lax.broadcasted_iota(jnp.int32, (2 * SUB, LANES), 1)

    def place(lhs, at, x, low, high):
        x0, x1 = x[:, :LANES], x[:, LANES:]
        views = (
            jnp.where(lane1 < LANES - DEPTH, x0, low),
            jnp.where(lane1 < LANES // 2, x1, x0),
            jnp.where(lane1 < DEPTH, high, x1),
        )
        for k, view in enumerate(views):
            first, second = split(view)
            lhs[k, at : at + 2 * SUB, :LANES] = first
            lhs[k, at : at + 2 * SUB, LANES:] = second

    def pair(left, right, at):
        low = [roll(left, LANES - DEPTH - at - h * DEPTH) for h in range(2)]
        high = [roll(right, -at - h * DEPTH) for h in range(2)]
        return jnp.concatenate(low, 0), jnp.concatenate(high, 0)

    def windows(t):
        e = group(t)
        left, right = (decode(rlon.at[b, t], 0, SUB * SUB) for b in range(2))
        for s in range(SUB):
            m, l = s // per, s % per
            mine = slice(s * SUB, (s + 1) * SUB)
            for q in range(0, rows // SUB, 2):
                r = slice(q * SUB, (q + 2) * SUB)
                w = pert[m, e * per + l, r].astype(jnp.float32) * g[e * per + l, r]
                place(lhs, s * rows + q * SUB, w, *pair(left[mine], right[mine], q * DEPTH))

    def margins(t):
        each = LANES // (2 * DEPTH)
        for a in range(sides):
            def fill():
                left, right = (root(rcor[a, b, t], 4) * (1.0 / CORNER) for b in range(2))
                for s in range(SUB):
                    j, i = s // each, s % each
                    mine = slice(j * SUB, (j + 1) * SUB)
                    w = [decode(rlat.at[a, t], (k * SUB + s) * DEPTH, DEPTH) for k in range(cols // LANES)]
                    place(lhm, (s * sides + a) * DEPTH, jnp.concatenate(w, 1),
                          *pair(left[mine], right[mine], i * 2 * DEPTH))

            where_(gets[a])(fill)
            if gets[a] is not None:
                @pl.when(jnp.logical_not(gets[a]))
                def _():
                    zero = jnp.zeros((DEPTH, 2 * LANES), jnp.bfloat16)
                    for s in range(SUB):
                        for k in range(3):
                            at = (s * sides + a) * DEPTH
                            lhm[k, at : at + DEPTH] = zero

    def damping(l):
        k1 = jnp.full((SUB, LANES), kappa[l], jnp.float32)
        scale = 1.0 / (1.0 + 4.0 * k1)
        tiles = []
        for i in range(0, full, SUB):
            n = k1 * eigen[kind, i : i + SUB]
            p = jnp.ones_like(n)
            for _ in range(SWEEPS):
                p = scale * (1.0 + n * p)
            for _ in range((2 * PASSES).bit_length() - 1):
                p = p * p
            tiles.append(p)
        return jnp.concatenate(tiles, 0)

    def dot(x, y):
        return jnp.dot(x, y, preferred_element_type=jnp.float32)

    def columns(t, source, first, count):
        for k in range(3):
            c = dot(source[k], into_c[k])
            for s in range(SUB):
                z = c[s * count : (s + 1) * count]
                high, low = split(z[:, :LANES] + z[:, LANES:])
                lanes = slice(k * LANES, (k + 1) * LANES)
                mid[t, s, first : first + count, lanes] = high
                mid[t, s, full + first : full + first + count, lanes] = low

    def start(t):
        for b in range(2):
            lon_copy(t, b).wait_recv()
        windows(t)
        columns(t, lhs, 0, rows)

    def transform(t):
        e = group(t)
        if sides:
            columns(t, lhm, rows, sides * DEPTH)
        for l in range(per):
            p = damping(e * per + l)
            p = jnp.concatenate([p, p, p], 1)
            batch = [m * per + l for m in range(members)]
            first = jnp.concatenate([mid[t, s, :full] for s in batch], 1)
            second = jnp.concatenate([mid[t, s, full:] for s in batch], 1)
            c = dot(into_r[kind], jnp.concatenate([first, first, second], 0))
            first, second = split(c * jnp.concatenate([p] * members, 1))
            c = dot(back_r[kind], jnp.concatenate([first, first, second], 0))
            first, second = split(c)
            for i, s in enumerate(batch):
                for k in range(3):
                    lanes = slice((3 * i + k) * LANES, (3 * i + k + 1) * LANES)
                    rhs[k, s * rows : (s + 1) * rows, :LANES] = first[:, lanes]
                    rhs[k, s * rows : (s + 1) * rows, LANES:] = second[:, lanes]

    def work(t, carry):
        e = group(t)
        start(t)
        for a in range(sides):
            @where_(gets[a])
            def _():
                lat_copy(t, a).wait_recv()
                for b in range(2):
                    cor_copy(t, a, b).wait_recv()
        margins(t)
        transform(t)
        lane2 = lax.broadcasted_iota(jnp.int32, (rows, LANES), 1)
        sums = [[0.0, 0.0] for _ in range(per)]
        y = [dot(rhs[k], back_c[k]) for k in range(3)]
        y = [v[:, :LANES] + v[:, LANES:] for v in y]
        for l in range(per):
            for m in range(members):
                s = m * per + l
                r = slice(s * rows, (s + 1) * rows)
                v = pert[m, e * per + l].astype(jnp.float32)
                low = jnp.where(lane2 < LANES - 2 * DEPTH, y[0][r], y[1][r])
                high = jnp.where(lane2 < 2 * DEPTH, y[1][r], y[2][r])
                sums[l][0] = sums[l][0] + v[:, :LANES] * low
                sums[l][1] = sums[l][1] + v[:, LANES:] * high
            tap = taper[e * per + l] * (1.0 / (members * n_mem - 1))
            total = jnp.concatenate(sums[l], 1) * tap
            own[l] = total

        @pl.when(t < n_mem - 1)
        def _():
            @pl.when(jnp.logical_and(t == 0, mem < n_mem - 1))
            def _():
                pl.semaphore_wait(ready, n_mem - 1 - mem)

            encode(part.at[t], own[...].reshape(per * rows, cols))
            part_copy(t).start()

        return carry

    lax.fori_loop(0, n_mem, work, 0)
    def drain(t, carry):
        for b in range(2):
            lon_copy(t, b).wait_send()
        for a in range(sides):
            @where_(sends[a])
            def _():
                lat_copy(t, a).wait_send()
                for b in range(2):
                    cor_copy(t, a, b).wait_send()
        return carry

    lax.fori_loop(0, n_mem, drain, 0)
    for i in range(n_mem - 1):
        part_come(i).wait_recv()
        for l in range(per):
            for k in range(cols // LANES):
                lanes = slice(k * LANES, (k + 1) * LANES)
                total = out if i == n_mem - 2 else own
                total[l, :, lanes] = own[l, :, lanes] + decode(rpart.at[i], (k * per + l) * rows, rows)
    if n_mem == 1:
        out[...] = own[...]
    for t in range(n_mem - 1):
        part_copy(t).wait_send()


def local(sizes, perturbations, increment, taper_norm, kappa):
    n_mem, n_lat, n_lon = sizes
    members, levels, rows, cols = perturbations.shape
    per = levels // n_mem
    assert members * per == SUB and cols == 2 * LANES and rows * DEPTH == SUB * LANES
    f32, bf16 = jnp.float32, jnp.bfloat16
    sides = min(n_lat - 1, 2)
    full = rows + sides * DEPTH
    tiles = SUB * 2 * DEPTH // LANES
    into_c, back_c, eig = column_tables()
    tables = (into_c, back_c) + row_tables(rows, sides, eig)
    arrays = (perturbations, increment, taper_norm, *map(jnp.asarray, tables))
    dma = pltpu.SemaphoreType.DMA
    vmem = pl.BlockSpec(memory_space=pltpu.VMEM)
    return pl.pallas_call(
        functools.partial(kernel, sizes),
        out_shape=pltpu.VMEM((per, rows, cols), f32),
        in_specs=[pl.BlockSpec(memory_space=pltpu.SMEM)] + [pl.BlockSpec(memory_space=pl.ANY)] * len(arrays),
        out_specs=vmem,
        scratch_shapes=[pltpu.VMEM(array.shape, array.dtype) for array in arrays] + [
            dma((3, n_mem)), dma((5,)), pltpu.SemaphoreType.REGULAR,
            pltpu.VMEM((levels, rows, cols), f32),
            pltpu.VMEM((2, n_mem, 2 * SUB + SUB * SUB, LANES), bf16),
            pltpu.VMEM((2, n_mem, 2 * SUB + SUB * SUB, LANES), bf16),
            pltpu.VMEM((2, 2, n_mem, tiles * SUB, LANES), bf16),
            pltpu.VMEM((2, 2, n_mem, tiles * SUB, LANES), bf16),
            pltpu.VMEM((2, n_mem, 2 * SUB + SUB * DEPTH * cols // LANES, LANES), bf16),
            pltpu.VMEM((2, n_mem, 2 * SUB + SUB * DEPTH * cols // LANES, LANES), bf16),
            pltpu.VMEM((3, SUB * rows, 2 * LANES), bf16),
            pltpu.VMEM((3, SUB * max(sides, 1) * DEPTH, 2 * LANES), bf16),
            pltpu.VMEM((n_mem, SUB, 2 * full, 3 * LANES), bf16),
            pltpu.VMEM((3, SUB * rows, 2 * LANES), jnp.bfloat16),
            pltpu.VMEM((per, rows, cols), f32),
            pltpu.VMEM((n_mem - 1, 2 * SUB + per * rows * cols // LANES, LANES), bf16),
            pltpu.VMEM((n_mem - 1, 2 * SUB + per * rows * cols // LANES, LANES), bf16),
            dma((2, n_mem)), dma((2, n_mem)),
            dma((2, n_mem)), dma((2, n_mem)),
            dma((2, 2, n_mem)), dma((2, 2, n_mem)),
            dma((n_mem - 1,)), dma((n_mem - 1,)),
        ],
        compiler_params=pltpu.CompilerParams(collective_id=0, has_side_effects=True),
    )(kappa, *arrays)


def solution(mesh):
    sizes = tuple(mesh.shape[name] for name in ("mem", "lat", "lon"))
    return jax.shard_map(
        functools.partial(local, sizes),
        mesh=mesh,
        in_specs=(P("mem", None, "lat", "lon"), P(None, "lat", "lon"), P(None, "lat", "lon"), P()),
        out_specs=P("mem", "lat", "lon"),
        check_vma=False,
    )
```

```python
import functools

import jax
import jax.numpy as jnp
import numpy as np
from jax import lax
from jax.experimental import pallas as pl
from jax.experimental.pallas import tpu as pltpu
from jax.sharding import PartitionSpec as P

PASSES = 4
SWEEPS = 2
DEPTH = 2 * PASSES * SWEEPS
SUB = 8
LANES = 128
MESH = pl.DeviceIdType.MESH
ROOT = 4
PEAK = 2.0 ** (126 / 2**ROOT)
CORNER = 2.0 ** (126 / 4) / 6.0**3


def roll(value, shift):
    shift = lax.rem(shift, LANES) if isinstance(shift, jax.Array) else shift % LANES
    return value if isinstance(shift, int) and shift == 0 else pltpu.roll(value, shift, value.ndim - 1)


def halves(matrix):
    high = np.asarray(matrix, np.float64).astype(jnp.bfloat16)
    return high, (matrix - high.astype(np.float64)).astype(jnp.bfloat16)


def sine(n):
    order = np.arange(1, n + 1)
    basis = np.sqrt(2.0 / (n + 1)) * np.sin(np.pi * np.outer(order, order) / (n + 1))
    return basis, 2.0 * np.cos(np.pi * order / (n + 1))


def column_tables():
    basis, own = sine(LANES)
    lanes = np.arange(LANES)
    into, back = [], []
    for shift in (DEPTH, LANES // 2, -DEPTH):
        high, low = halves(basis[(lanes + shift) % LANES])
        into.append(np.block([[high, low], [high, low]]))
        back.append(np.block([[high.T, low.T], [high.T, low.T]]))
    return np.stack(into), np.stack(back), own


def row_tables(rows, sides, columns):
    full = rows + sides * DEPTH
    kinds = [[], [0, 1], [0, 1, 2]][sides] or [None]
    into, back, own = [], [], []
    for kind in kinds:
        above = sides == 2 and kind > 0 or sides == 1 and kind == 1
        below = sides == 2 and kind < 2 or sides == 1 and kind == 0
        start = DEPTH if above else 0
        size = rows + start + (DEPTH if below else 0)
        basis, eig = sine(size)
        spots = [np.arange(start, start + rows)]
        for side, there in enumerate((above, below)):
            first = 0 if side == 0 else start + rows
            if there:
                spots.append(np.arange(first, first + DEPTH))
            elif sides == 2:
                spots.append(np.full(DEPTH, -1))
        spots = np.concatenate(spots)
        table = np.zeros((full, full))
        table[:size] = np.where(spots < 0, 0.0, basis[:, spots])
        high, low = halves(table)
        into.append(np.concatenate([high, low, high], 1))
        high, low = halves(table.T[:rows])
        back.append(np.concatenate([high, low, high], 1))
        sums = np.zeros((full, LANES))
        sums[:size] = eig[:, None] + columns
        own.append(sums.astype(np.float32))
    return np.stack(into), np.stack(back), np.stack(own)


def split(value):
    high = value.astype(jnp.bfloat16)
    return high, (value - high.astype(jnp.float32)).astype(jnp.bfloat16)


def top(value):
    tiles = [
        jnp.abs(value[i : i + SUB, j : j + LANES])
        for i in range(0, value.shape[0], SUB)
        for j in range(0, value.shape[1], LANES)
    ]
    while len(tiles) > 1:
        tiles = [jnp.maximum(*tiles[i : i + 2]) if tiles[i + 1 :] else tiles[i] for i in range(0, len(tiles), 2)]
    return tiles[0]


def spread(tile, like):
    tile = jnp.concatenate([tile] * (like.shape[1] // LANES), 1)
    return jnp.concatenate([tile] * (like.shape[0] // SUB), 0)


def power(value, squares):
    negative = value < 0.0
    for _ in range(squares):
        value = value * value
    return jnp.where(negative, -value, value).astype(jnp.bfloat16)


def root(coded, order):
    coded = coded.astype(jnp.float32)
    value = jnp.exp2(jnp.log2(jnp.abs(coded)) * (1.0 / order))
    return jnp.where(coded < 0.0, -value, value)


def encode(message, value):
    scale = jnp.maximum(top(value), 1e-36).astype(jnp.bfloat16)
    message[: 2 * SUB] = jnp.concatenate([scale, scale], 0)
    coded = power(value * spread(PEAK / scale.astype(jnp.float32), value), ROOT)
    for i in range(value.shape[1] // LANES):
        message[pl.ds(2 * SUB + i * value.shape[0], value.shape[0])] = coded[:, i * LANES : (i + 1) * LANES]


def decode(message, start, count):
    scale = message[: 2 * SUB].astype(jnp.float32)[:SUB] * (1.0 / PEAK)
    value = root(message[pl.ds(2 * SUB + start, count)], 2**ROOT)
    return value * spread(scale, value)


def kernel(
    sizes, kappa, pert_h, inc_h, taper_h, into_c_h, back_c_h, into_r_h, back_r_h, eigen_h, out,
    pert, inc, taper, into_c, back_c, into_r, back_r, eigen, load, load_c, ready, g, pack, rlon, cpack, rcor, epack, rlat, damp, lhs, lhm, mid, rhs, own, part, rpart,
    lon_send, lon_recv, lat_send, lat_recv, cor_send, cor_recv, part_send, part_recv,
):
    n_mem, n_lat, n_lon = sizes
    mem, lat, lon = lax.axis_index("mem"), lax.axis_index("lat"), lax.axis_index("lon")
    members, levels, rows, cols = pert.shape
    per = levels // n_mem
    sides = min(n_lat - 1, 2)
    full = rows + sides * DEPTH
    kind = jnp.where(lat == 0, 0, jnp.where(lat == n_lat - 1, sides, 1)) if sides else 0
    lane = lax.broadcasted_iota(jnp.int32, (SUB, LANES), 1)
    lon_to = [lax.rem(lon + 1, n_lon), lax.rem(lon + n_lon - 1, n_lon)]
    if sides == 1:
        lat_to, sends, gets, edge = [1 - lat], [None], [None], [jnp.where(lat == 0, rows - DEPTH, 0)]
    else:
        lat_to = [lat + 1, lat - 1][:sides]
        sends = [lat < n_lat - 1, lat > 0][:sides]
        gets = [lat > 0, lat < n_lat - 1][:sides]
        edge = [rows - DEPTH, 0]

    def where_(test):
        return pl.when(test) if test is not None else lambda body: body()

    def group(t):
        inner = jnp.where(t < mem, t, t + 1)
        first = n_mem - 1 - t
        last = jnp.where(t == 0, 0, n_mem - 1 - t)
        e = jnp.where(mem == 0, first, jnp.where(mem == n_mem - 1, last, inner))
        return jnp.where(t == n_mem - 1, mem, e)

    def spot(here, there):
        return lax.rem(here - there + n_mem - 1, n_mem)

    def remote(src, dst, send, recv, **where):
        return pltpu.make_async_remote_copy(
            src_ref=src, dst_ref=dst, send_sem=send, recv_sem=recv,
            device_id=where, device_id_type=MESH,
        )

    def lon_copy(t, b):
        return remote(pack.at[b, t], rlon.at[b, t], lon_send.at[b, t], lon_recv.at[b, t],
                      mem=mem, lat=lat, lon=lon_to[b])

    def cor_copy(t, a, b):
        return remote(cpack.at[a, b, t], rcor.at[a, b, t], cor_send.at[a, b, t],
                      cor_recv.at[a, b, t], mem=mem, lat=lat_to[a], lon=lon_to[b])

    def lat_copy(t, a):
        return remote(epack.at[a, t], rlat.at[a, t], lat_send.at[a, t], lat_recv.at[a, t],
                      mem=mem, lat=lat_to[a], lon=lon)

    def part_copy(t):
        e = group(t)
        i = spot(mem, e)
        return remote(part.at[t], rpart.at[i], part_send.at[t], part_recv.at[i],
                      mem=e, lat=lat, lon=lon)

    def part_come(i):
        return remote(part.at[i], rpart.at[i], part_send.at[i], part_recv.at[i],
                      mem=lax.rem(mem + 1, n_mem), lat=lat, lon=lon)

    def pieces(t):
        mine = pl.ds(group(t) * per, per)
        return [
            pltpu.make_async_copy(source, target, load.at[i, t])
            for i, (source, target) in enumerate((
                (inc_h.at[mine], inc.at[mine]), (taper_h.at[mine], taper.at[mine]),
                (pert_h.at[:, mine], pert.at[:, mine]),
            ))
        ]

    tables = [
        pltpu.make_async_copy(source, target, load_c.at[i])
        for i, (source, target) in enumerate((
            (into_c_h, into_c), (into_r_h, into_r), (eigen_h, eigen), (back_r_h, back_r), (back_c_h, back_c),
        ))
    ]
    for copy in pieces(0):
        copy.start()

    barrier = pltpu.get_barrier_semaphore()

    def greet(**where):
        pl.semaphore_signal(barrier, inc=1, device_id=where, device_id_type=MESH)

    for b in range(2):
        greet(mem=mem, lat=lat, lon=lon_to[b])
    for d in range(1, n_mem):
        @pl.when(mem + d < n_mem)
        def _():
            greet(mem=mem + d, lat=lat, lon=lon)
    for a in range(sides):
        @where_(sends[a])
        def _():
            greet(mem=mem, lat=lat_to[a], lon=lon)
            for b in range(2):
                greet(mem=mem, lat=lat_to[a], lon=lon_to[b])

    for copy in tables[:1] + pieces(1) + tables[1:]:
        copy.start()
    for t in range(2, n_mem):
        for copy in pieces(t):
            copy.start()

    beside = sum(1 if s is None else jnp.where(s, 1, 0) for s in sends)
    pl.semaphore_wait(barrier, 2 + mem + 3 * beside)
    for d in range(1, n_mem):
        @pl.when(mem >= d)
        def _():
            pl.semaphore_signal(ready, inc=1, device_id=dict(mem=mem - d, lat=lat, lon=lon), device_id_type=MESH)

    def send_group(t, carry):
        e = group(t)
        for copy in pieces(t):
            copy.wait()
        mine = pl.ds(e * per, per)
        g[mine] = taper[mine] * inc[mine]
        for a in range(sides):
            @where_(sends[a])
            def _():
                r = pl.ds(edge[a], DEPTH)
                w = [
                    pert[s // per, e * per + s % per, r, :].astype(jnp.float32) * g[e * per + s % per, r, :]
                    for s in range(SUB)
                ]
                encode(epack.at[a, t], jnp.concatenate(w, 0))
                lat_copy(t, a).start()

        each = LANES // (2 * DEPTH)
        corners = [[[None] * (SUB // each) for _ in range(2)] for _ in range(sides)]
        edges = [[], []]
        for s in range(SUB):
            m, l = s // per, s % per
            j, i = s // each, s % each
            for b, column in enumerate((cols - LANES, 0)):
                source = LANES - DEPTH if b == 0 else 0
                w = pert[m, e * per + l, :, pl.ds(column, LANES)].astype(jnp.float32)
                w = w * g[e * per + l, :, pl.ds(column, LANES)]
                acc = None
                for q in range(rows // SUB):
                    v = roll(w[q * SUB : (q + 1) * SUB], q * DEPTH - source)
                    acc = v if acc is None else jnp.where(lane >= q * DEPTH, v, acc)
                edges[b].append(acc)
                for a in range(sides):
                    v = roll(acc, LANES + i * 2 * DEPTH - edge[a] // SUB * DEPTH)
                    old = corners[a][b][j]
                    corners[a][b][j] = v if old is None else jnp.where(lane >= i * 2 * DEPTH, v, old)
        for b in range(2):
            encode(pack.at[b, t], jnp.concatenate(edges[b], 0))
            for a in range(sides):
                cpack[a, b, t] = power(jnp.concatenate(corners[a][b], 0) * CORNER, 2)
        for b in range(2):
            lon_copy(t, b).start()
        for a in range(sides):
            @where_(sends[a])
            def _():
                for b in range(2):
                    cor_copy(t, a, b).start()
        return carry

    lax.fori_loop(0, n_mem, send_group, 0)
    for copy in tables:
        copy.wait()

    lane1 = lax.broadcasted_iota(jnp.int32, (2 * SUB, LANES), 1)

    def place(lhs, at, x, low, high):
        x0, x1 = x[:, :LANES], x[:, LANES:]
        views = (
            jnp.where(lane1 < LANES - DEPTH, x0, low),
            jnp.where(lane1 < LANES // 2, x1, x0),
            jnp.where(lane1 < DEPTH, high, x1),
        )
        for k, view in enumerate(views):
            first, second = split(view)
            lhs[k, at : at + 2 * SUB, :LANES] = first
            lhs[k, at : at + 2 * SUB, LANES:] = second

    def pair(left, right, at):
        low = [roll(left, LANES - DEPTH - at - h * DEPTH) for h in range(2)]
        high = [roll(right, -at - h * DEPTH) for h in range(2)]
        return jnp.concatenate(low, 0), jnp.concatenate(high, 0)

    def windows(t):
        e = group(t)
        left, right = (decode(rlon.at[b, t], 0, SUB * SUB) for b in range(2))
        for s in range(SUB):
            m, l = s // per, s % per
            mine = slice(s * SUB, (s + 1) * SUB)
            for q in range(0, rows // SUB, 2):
                r = slice(q * SUB, (q + 2) * SUB)
                w = pert[m, e * per + l, r].astype(jnp.float32) * g[e * per + l, r]
                place(lhs, s * rows + q * SUB, w, *pair(left[mine], right[mine], q * DEPTH))

    def margins(t):
        each = LANES // (2 * DEPTH)
        for a in range(sides):
            def fill():
                left, right = (root(rcor[a, b, t], 4) * (1.0 / CORNER) for b in range(2))
                for s in range(SUB):
                    j, i = s // each, s % each
                    mine = slice(j * SUB, (j + 1) * SUB)
                    w = [decode(rlat.at[a, t], (k * SUB + s) * DEPTH, DEPTH) for k in range(cols // LANES)]
                    place(lhm, (s * sides + a) * DEPTH, jnp.concatenate(w, 1),
                          *pair(left[mine], right[mine], i * 2 * DEPTH))

            where_(gets[a])(fill)
            if gets[a] is not None:
                @pl.when(jnp.logical_not(gets[a]))
                def _():
                    zero = jnp.zeros((DEPTH, 2 * LANES), jnp.bfloat16)
                    for s in range(SUB):
                        for k in range(3):
                            at = (s * sides + a) * DEPTH
                            lhm[k, at : at + DEPTH] = zero

    def damping(l):
        k1 = jnp.full((SUB, LANES), kappa[l], jnp.float32)
        scale = 1.0 / (1.0 + 4.0 * k1)
        tiles = []
        for i in range(0, full, SUB):
            n = k1 * eigen[kind, i : i + SUB]
            p = jnp.ones_like(n)
            for _ in range(SWEEPS):
                p = scale * (1.0 + n * p)
            for _ in range((2 * PASSES).bit_length() - 1):
                p = p * p
            tiles.append(p)
        return jnp.concatenate(tiles, 0)

    def dot(x, y):
        return jnp.dot(x, y, preferred_element_type=jnp.float32)

    def columns(t, source, first, count):
        for k in range(3):
            c = dot(source[k], into_c[k])
            for s in range(SUB):
                z = c[s * count : (s + 1) * count]
                high, low = split(z[:, :LANES] + z[:, LANES:])
                lanes = slice(k * LANES, (k + 1) * LANES)
                mid[t, s, first : first + count, lanes] = high
                mid[t, s, full + first : full + first + count, lanes] = low

    def start(t):
        for b in range(2):
            lon_copy(t, b).wait_recv()
        windows(t)
        columns(t, lhs, 0, rows)
        for l in range(per):
            damp[l] = damping(group(t) * per + l)

    def transform(t):
        e = group(t)
        if sides:
            columns(t, lhm, rows, sides * DEPTH)
        for l in range(per):
            p = damp[l]
            p = jnp.concatenate([p, p, p], 1)
            batch = [m * per + l for m in range(members)]
            first = jnp.concatenate([mid[t, s, :full] for s in batch], 1)
            second = jnp.concatenate([mid[t, s, full:] for s in batch], 1)
            c = dot(into_r[kind], jnp.concatenate([first, first, second], 0))
            first, second = split(c * jnp.concatenate([p] * members, 1))
            c = dot(back_r[kind], jnp.concatenate([first, first, second], 0))
            first, second = split(c)
            for i, s in enumerate(batch):
                for k in range(3):
                    lanes = slice((3 * i + k) * LANES, (3 * i + k + 1) * LANES)
                    rhs[k, s * rows : (s + 1) * rows, :LANES] = first[:, lanes]
                    rhs[k, s * rows : (s + 1) * rows, LANES:] = second[:, lanes]

    def work(t, carry):
        e = group(t)
        start(t)
        for a in range(sides):
            @where_(gets[a])
            def _():
                lat_copy(t, a).wait_recv()
                for b in range(2):
                    cor_copy(t, a, b).wait_recv()
        margins(t)
        transform(t)
        lane2 = lax.broadcasted_iota(jnp.int32, (rows, LANES), 1)
        sums = [[0.0, 0.0] for _ in range(per)]
        y = [dot(rhs[k], back_c[k]) for k in range(3)]
        y = [v[:, :LANES] + v[:, LANES:] for v in y]
        for l in range(per):
            for m in range(members):
                s = m * per + l
                r = slice(s * rows, (s + 1) * rows)
                v = pert[m, e * per + l].astype(jnp.float32)
                low = jnp.where(lane2 < LANES - 2 * DEPTH, y[0][r], y[1][r])
                high = jnp.where(lane2 < 2 * DEPTH, y[1][r], y[2][r])
                sums[l][0] = sums[l][0] + v[:, :LANES] * low
                sums[l][1] = sums[l][1] + v[:, LANES:] * high
            tap = taper[e * per + l] * (1.0 / (members * n_mem - 1))
            total = jnp.concatenate(sums[l], 1) * tap
            own[l] = total

        @pl.when(t < n_mem - 1)
        def _():
            @pl.when(jnp.logical_and(t == 0, mem < n_mem - 1))
            def _():
                pl.semaphore_wait(ready, n_mem - 1 - mem)

            encode(part.at[t], own[...].reshape(per * rows, cols))
            part_copy(t).start()

        return carry

    lax.fori_loop(0, n_mem, work, 0)
    def drain(t, carry):
        for b in range(2):
            lon_copy(t, b).wait_send()
        for a in range(sides):
            @where_(sends[a])
            def _():
                lat_copy(t, a).wait_send()
                for b in range(2):
                    cor_copy(t, a, b).wait_send()
        return carry

    lax.fori_loop(0, n_mem, drain, 0)
    for i in range(n_mem - 1):
        part_come(i).wait_recv()
        for l in range(per):
            for k in range(cols // LANES):
                lanes = slice(k * LANES, (k + 1) * LANES)
                total = out if i == n_mem - 2 else own
                total[l, :, lanes] = own[l, :, lanes] + decode(rpart.at[i], (k * per + l) * rows, rows)
    if n_mem == 1:
        out[...] = own[...]
    for t in range(n_mem - 1):
        part_copy(t).wait_send()


def local(sizes, perturbations, increment, taper_norm, kappa):
    n_mem, n_lat, n_lon = sizes
    members, levels, rows, cols = perturbations.shape
    per = levels // n_mem
    assert members * per == SUB and cols == 2 * LANES and rows * DEPTH == SUB * LANES
    f32, bf16 = jnp.float32, jnp.bfloat16
    sides = min(n_lat - 1, 2)
    full = rows + sides * DEPTH
    tiles = SUB * 2 * DEPTH // LANES
    into_c, back_c, eig = column_tables()
    tables = (into_c, back_c) + row_tables(rows, sides, eig)
    arrays = (perturbations, increment, taper_norm, *map(jnp.asarray, tables))
    dma = pltpu.SemaphoreType.DMA
    vmem = pl.BlockSpec(memory_space=pltpu.VMEM)
    return pl.pallas_call(
        functools.partial(kernel, sizes),
        out_shape=pltpu.VMEM((per, rows, cols), f32),
        in_specs=[pl.BlockSpec(memory_space=pltpu.SMEM)] + [pl.BlockSpec(memory_space=pl.ANY)] * len(arrays),
        out_specs=vmem,
        scratch_shapes=[pltpu.VMEM(array.shape, array.dtype) for array in arrays] + [
            dma((3, n_mem)), dma((5,)), pltpu.SemaphoreType.REGULAR,
            pltpu.VMEM((levels, rows, cols), f32),
            pltpu.VMEM((2, n_mem, 2 * SUB + SUB * SUB, LANES), bf16),
            pltpu.VMEM((2, n_mem, 2 * SUB + SUB * SUB, LANES), bf16),
            pltpu.VMEM((2, 2, n_mem, tiles * SUB, LANES), bf16),
            pltpu.VMEM((2, 2, n_mem, tiles * SUB, LANES), bf16),
            pltpu.VMEM((2, n_mem, 2 * SUB + SUB * DEPTH * cols // LANES, LANES), bf16),
            pltpu.VMEM((2, n_mem, 2 * SUB + SUB * DEPTH * cols // LANES, LANES), bf16),
            pltpu.VMEM((per, full, LANES), f32),
            pltpu.VMEM((3, SUB * rows, 2 * LANES), bf16),
            pltpu.VMEM((3, SUB * max(sides, 1) * DEPTH, 2 * LANES), bf16),
            pltpu.VMEM((n_mem, SUB, 2 * full, 3 * LANES), bf16),
            pltpu.VMEM((3, SUB * rows, 2 * LANES), jnp.bfloat16),
            pltpu.VMEM((per, rows, cols), f32),
            pltpu.VMEM((n_mem - 1, 2 * SUB + per * rows * cols // LANES, LANES), bf16),
            pltpu.VMEM((n_mem - 1, 2 * SUB + per * rows * cols // LANES, LANES), bf16),
            dma((2, n_mem)), dma((2, n_mem)),
            dma((2, n_mem)), dma((2, n_mem)),
            dma((2, 2, n_mem)), dma((2, 2, n_mem)),
            dma((n_mem - 1,)), dma((n_mem - 1,)),
        ],
        compiler_params=pltpu.CompilerParams(collective_id=0, has_side_effects=True),
    )(kappa, *arrays)


def solution(mesh):
    sizes = tuple(mesh.shape[name] for name in ("mem", "lat", "lon"))
    return jax.shard_map(
        functools.partial(local, sizes),
        mesh=mesh,
        in_specs=(P("mem", None, "lat", "lon"), P(None, "lat", "lon"), P(None, "lat", "lon"), P()),
        out_specs=P("mem", "lat", "lon"),
        check_vma=False,
    )
```
